32 devices in a mesh: dp: 4 (over y, x), expert: 8 (over z, core).
Axes of the slice: x: 2, y: 2, z: 4, core: 2. Of those that a mesh axis runs over, the one named last changes fastest.
Arguments:
- tokens: bfloat16 [4096, 2048], P(('dp', 'expert')), may hold values from -6 to 6
- routes: int32 [4096, 8], P(('dp', 'expert')), may hold values from 0 to 15, all different within a row
- route_weight: float32 [4096, 8], P(('dp', 'expert')), may hold values from 0.05 to 0.5
- bias: float32 [16], replicated, may hold values from -3 to 3
- w_gate: bfloat16 [16, 768, 2048], P('expert', 'dp'), may hold values from -0.125 to 0.125
- w_up: bfloat16 [16, 768, 2048], P('expert', 'dp'), may hold values from -0.125 to 0.125
- w_down: bfloat16 [16, 768, 2048], P('expert', 'dp'), may hold values from -0.21875 to 0.21875
Outputs:
- mixed: bfloat16 [4096, 2048], P(('dp', 'expert'))
- new_bias: float32 [16], replicated
- counts: int32 [16], replicated
The draws below stay inside these ranges and needn't reach their ends.
Inputs may be any that keep to these rules, and one draw needn't show every extreme that they name: `routes`: each token names 8 different experts.
All inputs are finite; a program needn't handle non-finite values.
Results may differ from the reference program's by a relative error of at most 0.0057.
Values may be sent and summed in bfloat16 or wider, within the bound.
A program may use at most 128 MiB of HBM per device.

```python
import jax
import jax.numpy as jnp
from jax import lax

D = 2048
FF = 768
TOP = 8
TOK_DEV = 128
EXPERTS = 16
TOKENS = 4096
CAP = 80


def level_of(rng, extent, shards, smallest, top_value):
    loudness, own = 1.0, jax.random.fold_in(rng, 6)
    for position, shards_of in shards:
        heights = jnp.exp(jax.random.uniform(jax.random.fold_in(own, position), (shards_of,), jnp.float32, smallest / len(shards), top_value / len(shards)))
        loudness = loudness * jnp.repeat(heights, extent[position] // shards_of).reshape([-1 if axis == position else 1 for axis in range(len(extent))])
    return loudness


def different_ones(key, rows, amount, top, lift):
    order = jax.random.permutation(jax.random.fold_in(key, 1), amount)
    favour = order
    for power in range(3):
        favour = favour * favour // amount
    favour = favour * lift // amount
    lots = jax.random.randint(jax.random.fold_in(key, 2), (rows, amount), 0, 4096) + favour
    holders = jax.random.permutation(jax.random.fold_in(key, 3), rows)[jnp.arange(amount) % rows]
    lots = jnp.where(jnp.arange(rows)[:, None] == holders[None, :], 1 << 14, lots)
    merit = lots * amount + jnp.arange(amount)
    return lax.top_k(merit.astype(jnp.int32), top)[1].astype(jnp.int32)


def scatter_about(own_key, extent, width, reach, shards=(), held_as=jnp.bfloat16):
    drawn = jax.random.normal(own_key, extent, jnp.float32) * width
    if len(shards) > 0:
        drawn = level_of(own_key, extent, shards, -0.22, 0.18) * drawn
    return jnp.clip(drawn, min=-reach, max=reach).astype(held_as)


def setup_inputs(seed: int = 0) -> dict:
    key_of = jax.random.split(jax.random.key(seed), 8)
    tokens = scatter_about(key_of[0], (TOKENS, D), 1.0, 6.0, ((0, 32),))
    routes = different_ones(key_of[1], TOKENS, EXPERTS, TOP, 4096)
    route_weight = jnp.clip(0.05 + 0.45 * jax.random.uniform(key_of[2], (TOKENS, TOP), jnp.float32) ** level_of(key_of[2], (TOKENS, TOP), ((0, 32),), -0.2, 0.2), 0.05, 0.5)
    bias = scatter_about(key_of[3], (EXPERTS,), 0.5, 3.0, (), jnp.float32)
    w_gate = scatter_about(key_of[4], (EXPERTS, FF, D), D ** -0.5, 0.125, ((0, 8), (1, 4)))
    w_up = scatter_about(key_of[5], (EXPERTS, FF, D), D ** -0.5, 0.125, ((0, 8), (1, 4)))
    w_down = scatter_about(key_of[6], (EXPERTS, FF, D), FF ** -0.5, 0.21875, ((0, 8), (1, 4)))
    return dict(tokens=tokens, routes=routes, route_weight=route_weight, bias=bias, w_gate=w_gate, w_up=w_up, w_down=w_down)


bias_rate = 0.05


def reference(tokens, routes, route_weight, bias, w_gate, w_up, w_down):
    sources = TOKENS // TOK_DEV
    entries = TOK_DEV * TOP
    block_routes = routes.reshape(sources, entries)
    labels = jnp.arange(EXPERTS, dtype=jnp.int32)

    def rank_block(block_row):
        picked = (block_row[:, None] == labels[None, :]).astype(jnp.int32)
        running = jnp.cumsum(picked, axis=0) - picked
        return jnp.sum(running * picked, axis=1).astype(jnp.int32), jnp.sum(picked, axis=0).astype(jnp.int32)

    slot_rank, block_counts = lax.map(rank_block, block_routes)
    counts = jnp.sum(block_counts, axis=0).astype(jnp.int32)
    kept_mask = slot_rank < CAP
    source_index = jnp.arange(sources, dtype=jnp.int32)[:, None]
    token_index = (source_index * TOK_DEV + jnp.arange(entries, dtype=jnp.int32)[None, :] // TOP).astype(jnp.int32)
    slot_total = EXPERTS * sources * CAP
    slot_index = jnp.where(kept_mask, block_routes * (sources * CAP) + source_index * CAP + slot_rank, slot_total).astype(jnp.int32)
    token_table = jnp.zeros((slot_total + 1,), jnp.int32).at[slot_index.reshape(-1)].set(token_index.reshape(-1))
    token_table = token_table[:slot_total].reshape(EXPERTS, sources * CAP)
    entry_weight = jnp.where(kept_mask, route_weight.reshape(sources, entries), jnp.float32(0.0)).astype(jnp.float32)
    weight_table = jnp.zeros((slot_total + 1,), jnp.float32).at[slot_index.reshape(-1)].set(entry_weight.reshape(-1))
    weight_table = weight_table[:slot_total].reshape(EXPERTS, sources * CAP)

    def one_expert(carry_sum, expert_items):
        slot_tokens, slot_weights, gate_w, up_w, down_w = expert_items
        picked_rows = tokens[slot_tokens]
        gate_act = lax.dot_general(picked_rows, gate_w, (((1,), (1,)), ((), ())), preferred_element_type=jnp.float32)
        up_act = lax.dot_general(picked_rows, up_w, (((1,), (1,)), ((), ())), preferred_element_type=jnp.float32)
        hidden = (jax.nn.silu(gate_act) * up_act).astype(jnp.bfloat16)
        expert_out = jnp.dot(hidden, down_w, preferred_element_type=jnp.float32).astype(jnp.bfloat16)
        return carry_sum.at[slot_tokens].add(expert_out.astype(jnp.float32) * slot_weights[:, None]), None

    summed, _ = lax.scan(one_expert, jnp.zeros((TOKENS, D), jnp.float32), (token_table, weight_table, w_gate, w_up, w_down))
    mixed = summed.astype(jnp.bfloat16)
    new_bias = bias + bias_rate * jnp.sign((TOKENS * TOP - EXPERTS * counts).astype(jnp.float32))
    return mixed, new_bias, counts
```

```python
import functools

import jax
import jax.numpy as jnp
from jax import lax
from jax.experimental import pallas as pl
from jax.experimental.pallas import tpu as pltpu
from jax.sharding import PartitionSpec as P

bias_rate = 0.05
MESH = pl.DeviceIdType.MESH
VMEM_BYTES = 67043328
chunks = 16
lane_count = 128


def expert_products(received, gate_w, up_w, down_w):
    gate_act = jnp.einsum("sjcd,jfd->sjcf", received, gate_w, preferred_element_type=jnp.float32)
    up_act = jnp.einsum("sjcd,jfd->sjcf", received, up_w, preferred_element_type=jnp.float32)
    hidden = (jax.nn.silu(gate_act) * up_act).astype(jnp.bfloat16)
    return jnp.einsum("sjcf,jfd->sjcd", hidden, down_w, preferred_element_type=jnp.float32)


def exchange_body(tokens, routes, route_weight, bias, w_gate, w_up, w_down):
    tok_rows, feature_width = tokens.shape
    top_count = routes.shape[1]
    experts = bias.shape[0]
    groups = lax.axis_size("expert")
    per_device = w_gate.shape[0]
    capacity = 5 * tok_rows * top_count // (4 * experts)
    flat_routes = routes.reshape(-1)
    labels = jnp.arange(experts, dtype=jnp.int32)
    picked = (flat_routes[:, None] == labels[None, :]).astype(jnp.int32)
    running = jnp.cumsum(picked, axis=0) - picked
    slot_rank = jnp.sum(running * picked, axis=1)
    local_counts = jnp.sum(picked, axis=0)
    kept_mask = slot_rank < capacity
    slot_total = experts * capacity
    slot_index = jnp.where(kept_mask, flat_routes * capacity + slot_rank, slot_total)
    token_index = jnp.arange(tok_rows * top_count, dtype=jnp.int32) // top_count
    source = jnp.zeros((slot_total + 1,), jnp.int32).at[slot_index].set(token_index)[:slot_total]
    filled = jnp.zeros((slot_total + 1,), jnp.bool_).at[slot_index].set(True)[:slot_total]
    send_rows = jnp.where(filled[:, None], tokens[source], jnp.zeros((), jnp.bfloat16))
    send_rows = send_rows.reshape(groups, per_device, capacity, feature_width)
    gathered = [lax.all_gather(w, "dp", axis=1, tiled=True) for w in (w_gate, w_up, w_down)]
    produced = expert_products(
        lax.all_to_all(send_rows, "expert", split_axis=0, concat_axis=0, tiled=True), *gathered
    ).astype(jnp.bfloat16)
    returned = lax.all_to_all(produced, "expert", split_axis=0, concat_axis=0, tiled=True)
    flat_out = returned.reshape(slot_total, feature_width)
    fetched = flat_out[jnp.minimum(slot_index, slot_total - 1)]
    entry_weight = jnp.where(kept_mask, route_weight.reshape(-1), jnp.float32(0.0))
    weighted = fetched.astype(jnp.float32) * entry_weight[:, None]
    mixed = jnp.sum(weighted.reshape(tok_rows, top_count, feature_width), axis=1).astype(
        jnp.bfloat16
    )
    mean_load = tok_rows * top_count * lax.axis_size("dp") * groups
    totals = lax.psum(local_counts.astype(jnp.float32), ("dp", "expert"))
    new_bias = bias + bias_rate * jnp.sign(mean_load - experts * totals)
    return (mixed, new_bias, totals.astype(jnp.int32))


def layer_kernel(
    zs, capacity, per_device,
    tokens, routes_t, weights_t, w_gate, w_up, w_down,
    out, totals,
    tok, table, gate_w, up_w, down_w, scale, hidden, held,
    part1, keep1, recv1, part2, keep2, recv2, tally, tally_in,
    own_sem, own_d, tok_in, tok_out, tab_in, tab_out, w_in, w_out, d_in, d_out,
    m_in, m_out, md_in, md_out, f_in, f_out, fd_in, fd_out,
    s1_in, s1_out, s2_in, s2_out, t_in, t_out,
):
    rows, width = tokens.shape
    top = routes_t.shape[0]
    experts = table.shape[1] // 2
    pieces, lanes, _ = w_gate.shape
    ff = pieces * lanes
    unit = ff // per_device
    cd = width // chunks
    slots = tok.shape[0]
    dp, ex = lax.axis_index("dp"), lax.axis_index("expert")
    y, x = dp // 2, dp % 2
    z, c = ex // 2, ex % 2

    def at(y_, x_, z_, c_):
        return (y_ * 2 + x_, z_ * 2 + c_)

    def slot(y_, z_):
        return y_ * zs + z_

    def far(step):
        return lax.rem(z + step, zs)

    mate = at(y, x, z, 1 - c)
    y_side = at(1 - y, x, z, c)
    x_side = at(y, 1 - x, z, c)
    x_mate = at(y, 1 - x, z, 1 - c)
    me = slot(y, z)

    barrier = pltpu.get_barrier_semaphore()
    partners = [mate, y_side, x_side, x_mate] + [at(y, x, far(s), c) for s in range(1, zs)]
    for partner in partners:
        pl.semaphore_signal(barrier, inc=1, device_id=partner, device_id_type=MESH)

    def span(j):
        return pl.ds(pl.multiple_of(j * cd, cd), cd)

    own = [
        pltpu.make_async_copy(tokens, tok.at[me], own_sem.at[0]),
        pltpu.make_async_copy(w_gate, gate_w.at[0, :, 0], own_sem.at[1]),
        pltpu.make_async_copy(w_up, up_w.at[0, :, 0], own_sem.at[2]),
    ]
    for copy in own:
        copy.start()

    def own_down(j):
        return pltpu.make_async_copy(w_down.at[:, :, span(j)], down_w.at[j, 0, :, 0], own_d.at[j])

    labels = lax.broadcasted_iota(jnp.int32, (experts, rows), 0)
    picked = jnp.zeros((experts, rows), jnp.float32)
    weight = jnp.zeros((experts, rows), jnp.float32)
    for k in range(top):
        same = labels == routes_t[k : k + 1, :]
        picked += jnp.where(same, 1.0, 0.0)
        weight += jnp.where(same, weights_t[k : k + 1, :], 0.0)
    earlier = jnp.where(
        lax.broadcasted_iota(jnp.int32, (rows, rows), 0)
        < lax.broadcasted_iota(jnp.int32, (rows, rows), 1),
        1.0,
        0.0,
    )
    rank = jnp.dot(
        picked.astype(jnp.bfloat16),
        earlier.astype(jnp.bfloat16),
        preferred_element_type=jnp.float32,
    )
    table[me, 0:experts, :] = jnp.where(rank < capacity, weight, 0.0)
    table[me, experts : 2 * experts, :] = picked

    pl.semaphore_wait(barrier, len(partners))

    sent = []

    def remote(src, dst, ssem, rsem, device, keep=True):
        copy = pltpu.make_async_remote_copy(
            src_ref=src, dst_ref=dst, send_sem=ssem, recv_sem=rsem,
            device_id=device, device_id_type=MESH,
        )
        copy.start()
        if keep:
            sent.append(copy)

    def landed(ref, sem):
        pltpu.make_async_copy(ref, ref, sem).wait()

    def cross(n, p, source, target):
        remote(source.at[p], target.at[1, p, 0], w_out.at[n, p], w_in.at[n, p], x_side)

    def cross_down(j):
        remote(
            w_down.at[:, :, span(j)], down_w.at[j, 1, :, 0], d_out.at[j], d_in.at[j], x_side, False
        )

    for p in range(pieces):
        cross(0, p, w_gate, gate_w)
        if p == pieces - 1:
            cross_down(0)
        cross(1, p, w_up, up_w)

    def pass_on(n, index, device, source=None):
        remote(table.at[index], table.at[index], tab_out.at[n], tab_in.at[index], device, False)
        remote(
            tok.at[index] if source is None else source, tok.at[index],
            tok_out.at[n], tok_in.at[index], device, False,
        )

    def passed(n):
        pltpu.make_async_copy(table.at[0], table.at[0], tab_out.at[n]).wait()
        pltpu.make_async_copy(tok.at[0], tok.at[0], tok_out.at[n]).wait()

    def arrived(index):
        landed(table.at[index], tab_in.at[index])
        landed(tok.at[index], tok_in.at[index])

    above, below = z < zs - 1, z > 0
    z_up, z_down = at(y, x, z + 1, c), at(y, x, z - 1, c)

    @pl.when(above)
    def _():
        pass_on(z, me, z_up, tokens)

    @pl.when(below)
    def _():
        pass_on(zs + z, me, z_down, tokens)

    pass_on(2 * zs + z, me, y_side, tokens)

    remote(w_gate, gate_w.at[0, :, 1], m_out.at[0], m_in.at[0], mate)
    remote(w_up, up_w.at[0, :, 1], m_out.at[1], m_in.at[1], mate)

    def spread(j, carry):
        @pl.when(j > 0)
        def _():
            cross_down(j)

        own_down(j).start()
        remote(
            w_down.at[:, :, span(j)], down_w.at[j, 0, :, 1], md_out.at[j], md_in.at[j], mate, False
        )
        return carry

    lax.fori_loop(0, chunks, spread, 0)

    for copy in own:
        copy.wait()

    def relay(source, onward, device, n):
        index = slot(y, source)
        arrived(index)

        @pl.when(onward)
        def _():
            pass_on(n + source, index, device)

        pass_on(2 * zs + source, index, y_side)

    for d in range(1, zs):

        @pl.when(z >= d)
        def _():
            relay(z - d, above, z_up, 0)

        @pl.when(z + d < zs)
        def _():
            relay(z + d, below, z_down, zs)

    def forward(n, p, target):
        landed(target.at[1, p, 0], w_in.at[n, p])
        remote(target.at[1, p, 0], target.at[1, p, 1], f_out.at[n, p], f_in.at[n, p], mate)

    for p in range(pieces - 1):
        forward(0, p, gate_w)
        forward(1, p, up_w)

    def from_y(i, carry):
        arrived(slot(1 - y, i))
        return carry

    lax.fori_loop(0, zs, from_y, 0)

    def add_tally(i, total):
        return total + table[i, experts : 2 * experts, :]

    tally[...] = lax.fori_loop(0, slots, add_tally, jnp.zeros((experts, rows), jnp.float32))
    for i, device in enumerate((x_side, mate, x_mate)):
        remote(tally, tally_in.at[i], t_out.at[i], t_in.at[i], device)

    place = lax.broadcasted_iota(jnp.int32, (rows, lanes), 1)

    def fill(index, carry):
        for k in range(2):
            first = (z * 2 + (c if k == 0 else 1 - c)) * per_device
            columns = []
            for j in range(per_device):
                row = table[index, pl.ds(first + j, 1), :]
                columns.append(jnp.transpose(jnp.broadcast_to(row, (lanes, rows))))
            for p in range(pieces):
                piece = columns[0]
                for j in range(1, per_device):
                    piece = jnp.where(place + p * lanes >= j * unit, columns[j], piece)
                scale[p, index, :, k * lanes : (k + 1) * lanes] = piece
        return carry

    lax.fori_loop(0, slots, fill, 0)

    nt = (((1,), (1,)), ((), ()))
    pair = 2 * lanes

    def project(q, h, p, source):
        block = tok[pl.ds(q * zs, zs)].reshape(zs * rows, width)
        return lax.dot_general(
            block, source[h, p].reshape(pair, width), nt, preferred_element_type=jnp.float32
        )

    def activate(q, h, p, gate, up):
        value = gate / (1.0 + jnp.exp(-gate)) * up
        first = (h * pieces + p) * pair
        for i in range(zs):
            scaled = value[i * rows : (i + 1) * rows] * scale[p, q * zs + i]
            hidden[q * zs + i, :, first : first + pair] = scaled.astype(jnp.bfloat16)

    def both(h, p):
        def step(q, carry):
            activate(q, h, p, project(q, h, p, gate_w), project(q, h, p, up_w))
            return carry

        lax.fori_loop(0, 2, step, 0)

    landed(gate_w.at[0, :, 1], m_in.at[0])
    landed(up_w.at[0, :, 1], m_in.at[1])
    for p in range(pieces):
        both(0, p)
    for p in range(pieces - 1):
        landed(gate_w.at[1, p, 1], f_in.at[0, p])
        landed(up_w.at[1, p, 1], f_in.at[1, p])
        both(1, p)

    last = pieces - 1
    forward(0, last, gate_w)
    landed(gate_w.at[1, last, 1], f_in.at[0, last])

    def hold(q, carry):
        held[q] = project(q, 1, last, gate_w)
        return carry

    lax.fori_loop(0, 2, hold, 0)

    def fetch(j):
        landed(down_w.at[j, 1, :, 0], d_in.at[j])
        remote(
            down_w.at[j, 1, :, 0], down_w.at[j, 1, :, 1], fd_out.at[j], fd_in.at[j], mate, False
        )

    def ready(j):
        own_down(j).wait()
        landed(down_w.at[j, 0, :, 1], md_in.at[j])
        landed(down_w.at[j, 1, :, 1], fd_in.at[j])

    fetch(0)
    forward(1, last, up_w)
    ready(0)
    landed(up_w.at[1, last, 1], f_in.at[1, last])

    def finish(q):
        activate(q, 1, last, held[q], project(q, 1, last, up_w))

    def down(q, j):
        near = hidden[pl.ds(q * zs, zs)].reshape(zs * rows, 4 * ff)
        return jnp.dot(
            near, down_w[j].reshape(4 * ff, cd), preferred_element_type=jnp.float32
        ).reshape(zs, rows, cd)

    def away(j):
        part1[j] = down(1 - y, j).astype(jnp.bfloat16)
        remote(part1.at[j], recv1.at[j], s1_out.at[j], s1_in.at[j], y_side, False)

    def home(j):
        keep1[j] = down(y, j)

    def over_y(j):
        landed(recv1.at[j], s1_in.at[j])
        for s in range(1, zs):
            n = far(s)
            value = keep1[j, n] + recv1[j, n].astype(jnp.float32)
            part2[j, s - 1] = value.astype(jnp.bfloat16)
            remote(
                part2.at[j, s - 1], recv2.at[j, s - 1],
                s2_out.at[j, s - 1], s2_in.at[j, s - 1], at(y, x, n, c), False,
            )
        keep2[j] = keep1[j, z] + recv1[j, z].astype(jnp.float32)

    def over_z(j):
        value = keep2[j]
        for s in range(1, zs):
            landed(recv2.at[j, s - 1], s2_in.at[j, s - 1])
            value += recv2[j, s - 1].astype(jnp.float32)
        out[:, span(j)] = value.astype(jnp.bfloat16)

    finish(1 - y)
    away(0)
    finish(y)
    home(0)

    lag_y, lag_z = 2, 4

    def step(j, carry):
        fetch(j)
        ready(j)
        away(j)
        home(j)

        @pl.when(j >= lag_y)
        def _():
            over_y(j - lag_y)

        @pl.when(j >= lag_z)
        def _():
            over_z(j - lag_z)

        return carry

    lax.fori_loop(1, chunks, step, 0)

    def drain(j, carry):
        @pl.when(j < chunks + lag_y)
        def _():
            over_y(j - lag_y)

        over_z(j - lag_z)
        return carry

    lax.fori_loop(chunks, chunks + lag_z, drain, 0)

    count = tally[...]
    for i in range(3):
        landed(tally_in.at[i], t_in.at[i])
        count += tally_in[i]
    totals[...] = count
    for copy in sent:
        copy.wait_send()

    def gone(j, carry):
        @pl.when(j > 0)
        def _():
            landed(down_w.at[j, 1, :, 0], d_out.at[j])

        landed(down_w.at[j, 1, :, 0], md_out.at[j])
        landed(down_w.at[j, 1, :, 0], fd_out.at[j])
        landed(part1.at[j], s1_out.at[j])
        for s in range(1, zs):
            landed(part2.at[j, s - 1], s2_out.at[j, s - 1])
        return carry

    landed(down_w.at[0, 1, :, 0], d_out.at[0])
    lax.fori_loop(0, chunks, gone, 0)

    def z_sent(source, carry):
        @pl.when(jnp.logical_and(above, source <= z))
        def _():
            passed(source)

        @pl.when(jnp.logical_and(below, source >= z))
        def _():
            passed(zs + source)

        passed(2 * zs + source)
        return carry

    lax.fori_loop(0, zs, z_sent, 0)


def group_scratch(zs, rows, width, ff, experts):
    slots = 2 * zs
    cd = width // chunks
    pieces = ff // lane_count
    bf, f32 = jnp.bfloat16, jnp.float32
    return [
        ((slots, rows, width), bf),
        ((slots, 2 * experts, rows), f32),
        ((2, pieces, 2, lane_count, width), bf),
        ((2, pieces, 2, lane_count, width), bf),
        ((chunks, 2, pieces, 2, lane_count, cd), bf),
        ((pieces, slots, rows, 2 * lane_count), f32),
        ((slots, rows, 4 * ff), bf),
        ((2, zs * rows, 2 * lane_count), f32),
        ((chunks, zs, rows, cd), bf),
        ((chunks, zs, rows, cd), f32),
        ((chunks, zs, rows, cd), bf),
        ((chunks, zs - 1, rows, cd), bf),
        ((chunks, rows, cd), f32),
        ((chunks, zs - 1, rows, cd), bf),
        ((experts, rows), f32),
        ((3, experts, rows), f32),
    ]


def finish_kernel(load, mixed, tally, bias, out, new_bias, counts):
    out[...] = mixed[...]
    experts, rows = tally.shape
    row = lax.dot_general(
        jnp.ones((8, rows), jnp.bfloat16), tally[...].astype(jnp.bfloat16),
        (((1,), (1,)), ((), ())), preferred_element_type=jnp.float32,
    )[0:1]
    spare = load - experts * row
    step = jnp.where(spare > 0.0, bias_rate, jnp.where(spare < 0.0, -bias_rate, 0.0))
    new_bias[...] = bias[...] + step
    counts[...] = row.astype(jnp.int32)


def group_body(zs, tokens, routes, route_weight, bias, w_gate, w_up, w_down):
    rows, width = tokens.shape
    experts = bias.shape[0]
    per_device, unit, _ = w_gate.shape
    ff = per_device * unit
    top = routes.shape[1]
    capacity = 5 * rows * top // (4 * experts)
    slots = 2 * zs
    pieces = ff // lane_count
    dma = pltpu.SemaphoreType.DMA
    vmem = pl.BlockSpec(memory_space=pltpu.VMEM)
    anywhere = pl.BlockSpec(memory_space=pl.ANY)
    split = (pieces, lane_count, width)
    mixed, totals = pl.pallas_call(
        functools.partial(layer_kernel, zs, capacity, per_device),
        out_shape=(
            jax.ShapeDtypeStruct((rows, width), jnp.bfloat16),
            jax.ShapeDtypeStruct((experts, rows), jnp.float32),
        ),
        in_specs=[anywhere, vmem, vmem, anywhere, anywhere, anywhere],
        out_specs=(vmem, vmem),
        scratch_shapes=[
            pltpu.VMEM(shape, kind)
            for shape, kind in group_scratch(zs, rows, width, ff, experts)
        ]
        + [
            dma((3,)), dma((chunks,)),
            dma((slots,)), dma((3 * zs,)), dma((slots,)), dma((3 * zs,)),
            dma((2, pieces)), dma((2, pieces)), dma((chunks,)), dma((chunks,)),
            dma((2,)), dma((2,)), dma((chunks,)), dma((chunks,)),
            dma((2, pieces)), dma((2, pieces)), dma((chunks,)), dma((chunks,)),
            dma((chunks,)), dma((chunks,)), dma((chunks, zs - 1)), dma((chunks, zs - 1)),
            dma((3,)), dma((3,)),
        ],
        compiler_params=pltpu.CompilerParams(
            collective_id=0, has_side_effects=True, vmem_limit_bytes=VMEM_BYTES
        ),
    )(
        tokens, routes.T, route_weight.T,
        w_gate.reshape(split), w_up.reshape(split), w_down.reshape(split),
    )
    mean_load = rows * top * lax.axis_size("dp") * lax.axis_size("expert")
    mixed, new_bias, counts = pl.pallas_call(
        functools.partial(finish_kernel, mean_load),
        out_shape=(
            jax.ShapeDtypeStruct((rows, width), jnp.bfloat16),
            jax.ShapeDtypeStruct((1, experts), jnp.float32),
            jax.ShapeDtypeStruct((1, experts), jnp.int32),
        ),
        in_specs=[vmem, vmem, vmem],
        out_specs=(vmem, vmem, vmem),
    )(mixed, totals, bias.reshape(1, experts))
    return (mixed, new_bias.reshape(experts), counts.reshape(experts))


def body(tokens, routes, route_weight, bias, w_gate, w_up, w_down):
    rows, width = tokens.shape
    per_device, unit, _ = w_gate.shape
    ff = per_device * unit
    groups = lax.axis_size("expert")
    zs = groups // 2
    held = group_scratch(zs, rows, width, ff, bias.shape[0])
    total = 0
    for shape, kind in held:
        size = jnp.dtype(kind).itemsize
        for extent in shape:
            size *= extent
        total += size
    args = (tokens, routes, route_weight, bias, w_gate, w_up, w_down)
    fits = total < 0.85 * VMEM_BYTES and rows == lane_count
    even = ff % lane_count == 0 and width % (chunks * lane_count) == 0
    if lax.axis_size("dp") == 4 and groups % 2 == 0 and zs % 2 == 0 and fits and even:
        return group_body(zs, *args)
    return exchange_body(*args)


def solution(mesh):
    placed = (
        P(("dp", "expert"), None),
        P(("dp", "expert"), None),
        P(("dp", "expert"), None),
        P(),
        P("expert", "dp", None),
        P("expert", "dp", None),
        P("expert", "dp", None),
    )
    return jax.shard_map(
        body,
        mesh=mesh,
        in_specs=placed,
        out_specs=(P(("dp", "expert"), None), P(), P()),
        check_vma=False,
    )
```

```python
import functools

import jax
import jax.numpy as jnp
from jax import lax
from jax.experimental import pallas as pl
from jax.experimental.pallas import tpu as pltpu
from jax.sharding import PartitionSpec as P

bias_rate = 0.05
MESH = pl.DeviceIdType.MESH
VMEM_BYTES = 67043328
chunks = 16
lane_count = 128
crossed = (4, 8)
straight_chunks = 2


def expert_products(received, gate_w, up_w, down_w):
    gate_act = jnp.einsum("sjcd,jfd->sjcf", received, gate_w, preferred_element_type=jnp.float32)
    up_act = jnp.einsum("sjcd,jfd->sjcf", received, up_w, preferred_element_type=jnp.float32)
    hidden = (jax.nn.silu(gate_act) * up_act).astype(jnp.bfloat16)
    return jnp.einsum("sjcf,jfd->sjcd", hidden, down_w, preferred_element_type=jnp.float32)


def exchange_body(tokens, routes, route_weight, bias, w_gate, w_up, w_down):
    tok_rows, feature_width = tokens.shape
    top_count = routes.shape[1]
    experts = bias.shape[0]
    groups = lax.axis_size("expert")
    per_device = w_gate.shape[0]
    capacity = 5 * tok_rows * top_count // (4 * experts)
    flat_routes = routes.reshape(-1)
    labels = jnp.arange(experts, dtype=jnp.int32)
    picked = (flat_routes[:, None] == labels[None, :]).astype(jnp.int32)
    running = jnp.cumsum(picked, axis=0) - picked
    slot_rank = jnp.sum(running * picked, axis=1)
    local_counts = jnp.sum(picked, axis=0)
    kept_mask = slot_rank < capacity
    slot_total = experts * capacity
    slot_index = jnp.where(kept_mask, flat_routes * capacity + slot_rank, slot_total)
    token_index = jnp.arange(tok_rows * top_count, dtype=jnp.int32) // top_count
    source = jnp.zeros((slot_total + 1,), jnp.int32).at[slot_index].set(token_index)[:slot_total]
    filled = jnp.zeros((slot_total + 1,), jnp.bool_).at[slot_index].set(True)[:slot_total]
    send_rows = jnp.where(filled[:, None], tokens[source], jnp.zeros((), jnp.bfloat16))
    send_rows = send_rows.reshape(groups, per_device, capacity, feature_width)
    gathered = [lax.all_gather(w, "dp", axis=1, tiled=True) for w in (w_gate, w_up, w_down)]
    produced = expert_products(
        lax.all_to_all(send_rows, "expert", split_axis=0, concat_axis=0, tiled=True), *gathered
    ).astype(jnp.bfloat16)
    returned = lax.all_to_all(produced, "expert", split_axis=0, concat_axis=0, tiled=True)
    flat_out = returned.reshape(slot_total, feature_width)
    fetched = flat_out[jnp.minimum(slot_index, slot_total - 1)]
    entry_weight = jnp.where(kept_mask, route_weight.reshape(-1), jnp.float32(0.0))
    weighted = fetched.astype(jnp.float32) * entry_weight[:, None]
    mixed = jnp.sum(weighted.reshape(tok_rows, top_count, feature_width), axis=1).astype(
        jnp.bfloat16
    )
    mean_load = tok_rows * top_count * lax.axis_size("dp") * groups
    totals = lax.psum(local_counts.astype(jnp.float32), ("dp", "expert"))
    new_bias = bias + bias_rate * jnp.sign(mean_load - experts * totals)
    return (mixed, new_bias, totals.astype(jnp.int32))


def layer_kernel(
    zs, capacity, per_device,
    tokens, routes_t, weights_t, w_gate, w_up, w_down,
    out, totals,
    tok, table, gate_w, up_w, down_w, scale, hidden, held,
    part1, keep1, recv1, part2, keep2, recv2, far2, mix2,
    keep3, part3, recv3, far3, own3, mix3, part4, recv4, early, tally, tally_in,
    own_sem, own_d, tok_in, tok_out, tab_in, tab_out, w_in, w_out, d_in, d_out,
    m_in, m_out, md_in, md_out, f_in, f_out, fd_in, fd_out,
    s1_in, s1_out, s2_in, s2_out, c2_in, s3_in, s3_out, c3_in, s4_in, s4_out,
    t_in, t_out, turn,
):
    rows, width = tokens.shape
    top = routes_t.shape[0]
    experts = table.shape[1] // 2
    pieces, lanes, _ = w_gate.shape
    ff = pieces * lanes
    unit = ff // per_device
    cd = width // chunks
    slots = tok.shape[0]
    dp, ex = lax.axis_index("dp"), lax.axis_index("expert")
    y, x = dp // 2, dp % 2
    z, c = ex // 2, ex % 2

    def at(y_, x_, z_, c_):
        return (y_ * 2 + x_, z_ * 2 + c_)

    def slot(y_, z_):
        return y_ * zs + z_

    def far(step):
        return lax.rem(z + step, zs)

    mate = at(y, x, z, 1 - c)
    y_side = at(1 - y, x, z, c)
    x_side = at(y, 1 - x, z, c)
    x_mate = at(y, 1 - x, z, 1 - c)
    me = slot(y, z)

    barrier = pltpu.get_barrier_semaphore()
    partners = [mate, y_side, x_side, x_mate] + [at(y, x, far(s), c) for s in range(1, zs)]
    for partner in partners:
        pl.semaphore_signal(barrier, inc=1, device_id=partner, device_id_type=MESH)

    def span(j):
        return pl.ds(pl.multiple_of(j * cd, cd), cd)

    own = [
        pltpu.make_async_copy(tokens, tok.at[me], own_sem.at[0]),
        pltpu.make_async_copy(w_gate, gate_w.at[0, :, 0], own_sem.at[1]),
        pltpu.make_async_copy(w_up, up_w.at[0, :, 0], own_sem.at[2]),
    ]
    for copy in own:
        copy.start()

    def own_down(j):
        return pltpu.make_async_copy(w_down.at[:, :, span(j)], down_w.at[j, 0, :, 0], own_d)

    labels = lax.broadcasted_iota(jnp.int32, (experts, rows), 0)
    picked = jnp.zeros((experts, rows), jnp.float32)
    weight = jnp.zeros((experts, rows), jnp.float32)
    for k in range(top):
        same = labels == routes_t[k : k + 1, :]
        picked += jnp.where(same, 1.0, 0.0)
        weight += jnp.where(same, weights_t[k : k + 1, :], 0.0)
    earlier = jnp.where(
        lax.broadcasted_iota(jnp.int32, (rows, rows), 0)
        < lax.broadcasted_iota(jnp.int32, (rows, rows), 1),
        1.0,
        0.0,
    )
    rank = jnp.dot(
        picked.astype(jnp.bfloat16),
        earlier.astype(jnp.bfloat16),
        preferred_element_type=jnp.float32,
    )
    table[me, 0:experts, :] = jnp.where(rank < capacity, weight, 0.0)
    table[me, experts : 2 * experts, :] = picked

    pl.semaphore_wait(barrier, len(partners))

    def remote(src, dst, ssem, rsem, device):
        copy = pltpu.make_async_remote_copy(
            src_ref=src, dst_ref=dst, send_sem=ssem, recv_sem=rsem,
            device_id=device, device_id_type=MESH,
        )
        copy.start()
        return copy

    def landed(ref, sem):
        pltpu.make_async_copy(ref, ref, sem).wait()

    def cross(n, p, source, target):
        final = n == 1 and p == pieces - 1
        return remote(
            source.at[p], target.at[1, p, 0], w_out.at[1 if final else 0], w_in.at[n, p],
            x_side,
        )

    def cross_down(j):
        remote(
            w_down.at[:, :, span(j)], down_w.at[j, 1, :, 0], d_out, d_in.at[j], x_side
        )

    for p in range(pieces):
        cross(0, p, w_gate, gate_w)
        if p == pieces - 1:
            cross_down(0)
        last_up = cross(1, p, w_up, up_w)

    def pass_on(n, index, device, source=None):
        remote(table.at[index], table.at[index], tab_out.at[n], tab_in.at[index], device)
        remote(
            tok.at[index] if source is None else source, tok.at[index],
            tok_out.at[n], tok_in.at[index], device,
        )

    def passed(n, count):
        landed(table.at[pl.ds(0, count)], tab_out.at[n])
        landed(tok.at[pl.ds(0, count)], tok_out.at[n])

    def arrived(index):
        landed(table.at[index], tab_in.at[index])
        landed(tok.at[index], tok_in.at[index])

    above, below = z < zs - 1, z > 0
    z_up, z_down = at(y, x, z + 1, c), at(y, x, z - 1, c)

    @pl.when(above)
    def _():
        pass_on(0, me, z_up, tokens)

    @pl.when(below)
    def _():
        pass_on(0, me, z_down, tokens)

    pass_on(1, me, y_side, tokens)

    remote(w_gate, gate_w.at[0, :, 1], m_out, m_in.at[0], mate)
    remote(w_up, up_w.at[0, :, 1], m_out, m_in.at[1], mate)

    def spread(j, carry):
        own_down(j).start()
        remote(
            w_down.at[:, :, span(j)], down_w.at[j, 0, :, 1], md_out, md_in, mate
        )
        return carry

    lax.fori_loop(0, chunks, spread, 0)

    for copy in own:
        copy.wait()

    def relay(source, onward, device):
        index = slot(y, source)
        arrived(index)

        @pl.when(onward)
        def _():
            pass_on(0, index, device)

        pass_on(1, index, y_side)

    for d in range(1, zs):

        @pl.when(z >= d)
        def _():
            relay(z - d, above, z_up)

        @pl.when(z + d < zs)
        def _():
            relay(z + d, below, z_down)

    def forward(n, p, target):
        landed(target.at[1, p, 0], w_in.at[n, p])
        remote(target.at[1, p, 0], target.at[1, p, 1], f_out, f_in.at[n, p], mate)

    for p in range(pieces - 1):
        forward(0, p, gate_w)
        forward(1, p, up_w)

    def from_y(i, carry):
        arrived(slot(1 - y, i))
        return carry

    lax.fori_loop(0, zs, from_y, 0)

    def add_tally(i, total):
        return total + table[i, experts : 2 * experts, :]

    tally[...] = lax.fori_loop(0, slots, add_tally, jnp.zeros((experts, rows), jnp.float32))
    for i, device in enumerate((x_side, mate, x_mate)):
        remote(tally, tally_in.at[i], t_out, t_in.at[i], device)

    place = lax.broadcasted_iota(jnp.int32, (rows, lanes), 1)

    def fill(index, carry):
        for k in range(2):
            first = (z * 2 + (c if k == 0 else 1 - c)) * per_device
            columns = []
            for j in range(per_device):
                row = table[index, pl.ds(first + j, 1), :]
                columns.append(jnp.transpose(jnp.broadcast_to(row, (lanes, rows))))
            for p in range(pieces):
                piece = columns[0]
                for j in range(1, per_device):
                    piece = jnp.where(place + p * lanes >= j * unit, columns[j], piece)
                scale[p, index, :, k * lanes : (k + 1) * lanes] = piece
        return carry

    lax.fori_loop(0, slots, fill, 0)

    nt = (((1,), (1,)), ((), ()))
    pair = 2 * lanes

    def project(q, h, p, source):
        block = tok[pl.ds(q * zs, zs)].reshape(zs * rows, width)
        return lax.dot_general(
            block, source[h, p].reshape(pair, width), nt, preferred_element_type=jnp.float32
        )

    def gated(q, p, gate):
        value = gate / (1.0 + jnp.exp(-gate))
        factor = scale[p, pl.ds(q * zs, zs)].reshape(zs * rows, pair)
        return value * factor

    def activate(q, h, p, gate, up):
        first = (h * pieces + p) * pair
        value = (gate * up).astype(jnp.bfloat16)
        hidden[pl.ds(q * zs, zs), :, first : first + pair] = value.reshape(zs, rows, pair)

    def both(h, p):
        def step(q, carry):
            gate = gated(q, p, project(q, h, p, gate_w))
            activate(q, h, p, gate, project(q, h, p, up_w))
            return carry

        lax.fori_loop(0, 2, step, 0)

    landed(gate_w.at[0, :, 1], m_in.at[0])
    landed(up_w.at[0, :, 1], m_in.at[1])
    for p in range(pieces):
        both(0, p)
    for p in range(pieces - 1):
        landed(gate_w.at[1, p, 1], f_in.at[0, p])
        landed(up_w.at[1, p, 1], f_in.at[1, p])
        both(1, p)

    last = pieces - 1
    forward(0, last, gate_w)
    landed(gate_w.at[1, last, 1], f_in.at[0, last])

    def hold(q, carry):
        held[q] = gated(q, last, project(q, 1, last, gate_w))
        return carry

    lax.fori_loop(0, 2, hold, 0)

    def fetch(j):
        landed(down_w.at[j, 1, :, 0], d_in.at[j])
        remote(
            down_w.at[j, 1, :, 0], down_w.at[j, 1, :, 1], fd_out, fd_in.at[j], mate
        )

    def ready(j):
        landed(down_w.at[j, 1, :, 1], fd_in.at[j])

    fetch(0)
    landed(down_w.at[:, 0, :, 0], own_d)
    landed(down_w.at[:, 0, :, 1], md_in)
    ready(0)
    known = 4 * ff - pair

    def begin(q, carry):
        near = hidden[pl.ds(q * zs, zs), :, 0:known].reshape(zs * rows, known)
        weights = down_w[0].reshape(4 * ff, cd)[0:known]
        early[q] = jnp.dot(near, weights, preferred_element_type=jnp.float32)
        return carry

    lax.fori_loop(0, 2, begin, 0)

    last_up.wait_send()
    pl.semaphore_signal(turn, inc=1, device_id=mate, device_id_type=MESH)
    pl.semaphore_wait(turn, 1)

    def follow(j, carry):
        cross_down(j)
        return carry

    lax.fori_loop(1, chunks, follow, 0)
    forward(1, last, up_w)
    landed(up_w.at[1, last, 1], f_in.at[1, last])

    def finish(q):
        block = tok[pl.ds(q * zs, zs)].reshape(zs * rows, width)
        part = up_w[1, last].reshape(pair, width)
        half = width // 2
        ups = [
            lax.dot_general(
                block[:, k * half : (k + 1) * half], part[:, k * half : (k + 1) * half],
                nt, preferred_element_type=jnp.float32,
            )
            for k in range(2)
        ]
        activate(q, 1, last, held[q], ups[0] + ups[1])

    def down(q, j):
        near = hidden[pl.ds(q * zs, zs)].reshape(zs * rows, 4 * ff)
        return jnp.dot(
            near, down_w[j].reshape(4 * ff, cd), preferred_element_type=jnp.float32
        ).reshape(zs, rows, cd)

    def down_first(q):
        near = hidden[pl.ds(q * zs, zs), :, known : 4 * ff].reshape(zs * rows, pair)
        weights = down_w[0].reshape(4 * ff, cd)[known : 4 * ff]
        value = early[q] + jnp.dot(near, weights, preferred_element_type=jnp.float32)
        return value.reshape(zs, rows, cd)

    def away(j, value):
        part1[j] = value.astype(jnp.bfloat16)
        remote(part1.at[j], recv1.at[j], s1_out, s1_in.at[j], y_side)

    end = jnp.logical_or(z == 0, z == zs - 1)
    inner = jnp.logical_not(end)
    beside = z + 1 - 2 * lax.rem(z, 2)
    across = lax.rem(z + 2, zs)
    mirror = zs - 1 - z
    straight = jnp.where(end, across, mirror)
    lane = jnp.where(end, 1, 2)

    def out_z(j, value, part, recv, kept, mix, outs, ins, mix_in, direct=None):
        def send(i, n, target, sem, device):
            part[j, i] = value(n).astype(jnp.bfloat16)
            remote(part.at[j, i], target, outs, sem, at(y, x, device, c))

        send(0, beside, recv.at[j, 0], ins.at[j], beside)
        send(1, straight, recv.at[j, lane], ins.at[j], straight)

        def relayed():
            @pl.when(end)
            def _():
                send(2, mirror, mix.at[j], mix_in.at[j], beside)

            @pl.when(inner)
            def _():
                kept[j] = value(across)

        def unrelayed():
            @pl.when(end)
            def _():
                send(2, mirror, recv.at[j, 2], ins.at[j], mirror)

            @pl.when(inner)
            def _():
                send(2, across, recv.at[j, 1], ins.at[j], across)

        if direct is None:
            relayed()
        else:
            pl.when(direct)(unrelayed)
            pl.when(jnp.logical_not(direct))(relayed)

    def merge(j, part, recv, kept, mix, outs, ins, mix_in):
        @pl.when(inner)
        def _():
            landed(mix.at[j], mix_in.at[j])
            part[j, 2] = (kept[j] + mix[j].astype(jnp.float32)).astype(jnp.bfloat16)
            remote(
                part.at[j, 2], recv.at[j, 1], outs, ins.at[j],
                at(y, x, across, c),
            )

    def in_z(j, total, recv, ins, third):
        def add(count):
            landed(recv.at[j, pl.ds(0, count)], ins.at[j])
            value = total[j]
            for i in range(count):
                value = value + recv[j, i].astype(jnp.float32)
            total[j] = value

        pl.when(third)(lambda: add(3))
        pl.when(jnp.logical_not(third))(lambda: add(2))

    def is_last(j):
        return j >= chunks - straight_chunks

    def over_y(j):
        landed(recv1.at[j], s1_in.at[j])

        def value(n):
            return keep1[j, n] + recv1[j, n].astype(jnp.float32)

        out_z(j, value, part2, recv2, far2, mix2, s2_out, s2_in, c2_in, is_last(j))
        keep2[j] = value(z)

    def merge_y(j):
        merge(j, part2, recv2, far2, mix2, s2_out, s2_in, c2_in)

    def over_z(j):
        in_z(j, keep2, recv2, s2_in, jnp.logical_or(inner, is_last(j)))
        out[:, span(j)] = keep2[j].astype(jnp.bfloat16)

    def first_z(b):
        def value(n):
            return keep3[b, :, n]

        out_z(b, value, part3, recv3, far3, mix3, s3_out, s3_in, c3_in)
        own3[b] = value(z)

    def then_y(b):
        in_z(b, own3, recv3, s3_in, inner)
        part4[b] = own3[b, 1 - y].astype(jnp.bfloat16)
        remote(part4.at[b], recv4.at[b], s4_out, s4_in.at[b], y_side)

    def crossed_out(b, j):
        landed(recv4.at[b], s4_in.at[b])
        value = own3[b, y] + recv4[b].astype(jnp.float32)
        out[:, span(j)] = value.astype(jnp.bfloat16)

    finish(1 - y)
    away(0, down_first(1 - y))
    fetch(1)
    finish(y)
    keep1[0] = down_first(y)

    lag_y, lag_m, lag_z = 2, 6, 10
    late = chunks - straight_chunks - 3

    def plain(j):
        ok = jnp.logical_and(j >= 0, j < chunks)
        for special in crossed:
            ok = jnp.logical_and(ok, j != special)
        return ok

    def step(j, carry):
        @pl.when(j < chunks)
        def _():
            ready(j)

            @pl.when(plain(j))
            def _():
                away(j, down(1 - y, j))

            for b, special in enumerate(crossed):

                @pl.when(j == special)
                def _(b=b):
                    keep3[b, 1 - y] = down(1 - y, j)

            @pl.when(j < chunks - 1)
            def _():
                fetch(j + 1)

            @pl.when(plain(j))
            def _():
                keep1[j] = down(y, j)

            for b, special in enumerate(crossed):

                @pl.when(j == special)
                def _(b=b):
                    keep3[b, y] = down(y, j)
                    first_z(b)

        for lag, first, past in (
            (lag_m, 0, late), (lag_m - 2, late, chunks - straight_chunks)
        ):
            due = jnp.logical_and(j - lag >= first, j - lag < past)

            @pl.when(jnp.logical_and(plain(j - lag), due))
            def _(lag=lag):
                merge_y(j - lag)

        @pl.when(plain(j - lag_y))
        def _():
            over_y(j - lag_y)

        for b, special in enumerate(crossed):

            @pl.when(j == special + 5)
            def _(b=b):
                merge(b, part3, recv3, far3, mix3, s3_out, s3_in, c3_in)

            @pl.when(j == special + 7)
            def _(b=b):
                then_y(b)

            @pl.when(j == special + 11)
            def _(b=b, special=special):
                crossed_out(b, special)

        @pl.when(plain(j - lag_z))
        def _():
            over_z(j - lag_z)

        return carry

    lax.fori_loop(1, chunks + lag_z, step, 0)

    count = tally[...]
    for i in range(3):
        landed(tally_in.at[i], t_in.at[i])
        count += tally_in[i]
    totals[...] = count
    landed(gate_w.at[:, :, 1], m_out)
    landed(gate_w.at[:, :, 1], f_out)
    landed(tok.at[pl.ds(0, 2 * pieces - 1)], w_out.at[0])
    landed(tally_in, t_out)

    for sem in (d_out, md_out, fd_out):
        landed(down_w.at[:, 1, :, 0], sem)
    usual = pl.ds(0, chunks - len(crossed))
    landed(part1.at[usual], s1_out)
    landed(part2.at[usual], s2_out)
    landed(part3, s3_out)
    landed(part4, s4_out)

    passed(1, zs)

    @pl.when(end)
    def _():
        passed(0, 1)

    @pl.when(inner)
    def _():
        passed(0, zs + 1)


def group_scratch(zs, rows, width, ff, experts):
    slots = 2 * zs
    cd = width // chunks
    pieces = ff // lane_count
    twice = len(crossed)
    bf, f32 = jnp.bfloat16, jnp.float32
    return [
        ((slots, rows, width), bf),
        ((slots, 2 * experts, rows), f32),
        ((2, pieces, 2, lane_count, width), bf),
        ((2, pieces, 2, lane_count, width), bf),
        ((chunks, 2, pieces, 2, lane_count, cd), bf),
        ((pieces, slots, rows, 2 * lane_count), f32),
        ((slots, rows, 4 * ff), bf),
        ((2, zs * rows, 2 * lane_count), f32),
        ((chunks, zs, rows, cd), bf),
        ((chunks, zs, rows, cd), f32),
        ((chunks, zs, rows, cd), bf),
        ((chunks, zs - 1, rows, cd), bf),
        ((chunks, rows, cd), f32),
        ((chunks, zs - 1, rows, cd), bf),
        ((chunks, rows, cd), f32),
        ((chunks, rows, cd), bf),
        ((twice, 2, zs, rows, cd), f32),
        ((twice, zs - 1, 2, rows, cd), bf),
        ((twice, zs - 1, 2, rows, cd), bf),
        ((twice, 2, rows, cd), f32),
        ((twice, 2, rows, cd), f32),
        ((twice, 2, rows, cd), bf),
        ((twice, rows, cd), bf),
        ((twice, rows, cd), bf),
        ((2, zs * rows, cd), f32),
        ((experts, rows), f32),
        ((3, experts, rows), f32),
    ]


def finish_kernel(load, mixed, tally, bias, out, new_bias, counts, done):
    copy = pltpu.make_async_copy(mixed, out, done)
    copy.start()
    experts, rows = tally.shape
    row = lax.dot_general(
        jnp.ones((8, rows), jnp.bfloat16), tally[...].astype(jnp.bfloat16),
        (((1,), (1,)), ((), ())), preferred_element_type=jnp.float32,
    )[0:1]
    spare = load - experts * row
    step = jnp.where(spare > 0.0, bias_rate, jnp.where(spare < 0.0, -bias_rate, 0.0))
    new_bias[...] = bias[...] + step
    counts[...] = row.astype(jnp.int32)
    copy.wait()


def group_body(zs, tokens, routes, route_weight, bias, w_gate, w_up, w_down):
    rows, width = tokens.shape
    experts = bias.shape[0]
    per_device, unit, _ = w_gate.shape
    ff = per_device * unit
    top = routes.shape[1]
    capacity = 5 * rows * top // (4 * experts)
    slots = 2 * zs
    pieces = ff // lane_count
    twice = len(crossed)
    dma = pltpu.SemaphoreType.DMA
    vmem = pl.BlockSpec(memory_space=pltpu.VMEM)
    anywhere = pl.BlockSpec(memory_space=pl.ANY)
    split = (pieces, lane_count, width)
    mixed, totals = pl.pallas_call(
        functools.partial(layer_kernel, zs, capacity, per_device),
        out_shape=(
            pltpu.VMEM((rows, width), jnp.bfloat16),
            pltpu.VMEM((experts, rows), jnp.float32),
        ),
        in_specs=[anywhere, vmem, vmem, anywhere, anywhere, anywhere],
        out_specs=(vmem, vmem),
        scratch_shapes=[
            pltpu.VMEM(shape, kind)
            for shape, kind in group_scratch(zs, rows, width, ff, experts)
        ]
        + [
            dma((3,)), dma, dma((slots,)), dma((2,)), dma((slots,)), dma((2,)),
            dma((2, pieces)), dma((2,)), dma((chunks,)), dma, dma((2,)), dma, dma, dma,
            dma((2, pieces)), dma, dma((chunks,)), dma,
            dma((chunks,)), dma, dma((chunks,)), dma,
            dma((chunks,)), dma((twice,)), dma, dma((twice,)),
            dma((twice,)), dma, dma((3,)), dma, pltpu.SemaphoreType.REGULAR,
        ],
        compiler_params=pltpu.CompilerParams(
            collective_id=0, has_side_effects=True, vmem_limit_bytes=60000000
        ),
    )(
        tokens, routes.T, route_weight.T,
        w_gate.reshape(split), w_up.reshape(split), w_down.reshape(split),
    )
    mixed = pltpu.with_memory_space_constraint(mixed, pltpu.VMEM)
    totals = pltpu.with_memory_space_constraint(totals, pltpu.VMEM)
    mean_load = rows * top * lax.axis_size("dp") * lax.axis_size("expert")
    mixed, new_bias, counts = pl.pallas_call(
        functools.partial(finish_kernel, mean_load),
        out_shape=(
            jax.ShapeDtypeStruct((rows, width), jnp.bfloat16),
            jax.ShapeDtypeStruct((1, experts), jnp.float32),
            jax.ShapeDtypeStruct((1, experts), jnp.int32),
        ),
        in_specs=[vmem, vmem, vmem],
        out_specs=(anywhere, vmem, vmem),
        scratch_shapes=[dma],
    )(mixed, totals, bias.reshape(1, experts))
    return (mixed, new_bias.reshape(experts), counts.reshape(experts))


def body(tokens, routes, route_weight, bias, w_gate, w_up, w_down):
    rows, width = tokens.shape
    per_device, unit, _ = w_gate.shape
    ff = per_device * unit
    groups = lax.axis_size("expert")
    zs = groups // 2
    held = group_scratch(zs, rows, width, ff, bias.shape[0])
    total = 0
    for shape, kind in held:
        size = jnp.dtype(kind).itemsize
        for extent in shape:
            size *= extent
        total += size
    args = (tokens, routes, route_weight, bias, w_gate, w_up, w_down)
    fits = total < 0.85 * VMEM_BYTES and rows == lane_count
    even = ff % lane_count == 0 and width % (chunks * lane_count) == 0
    if lax.axis_size("dp") == 4 and groups % 2 == 0 and zs == 4 and fits and even:
        return group_body(zs, *args)
    return exchange_body(*args)


def solution(mesh):
    placed = (
        P(("dp", "expert"), None),
        P(("dp", "expert"), None),
        P(("dp", "expert"), None),
        P(),
        P("expert", "dp", None),
        P("expert", "dp", None),
        P("expert", "dp", None),
    )
    return jax.shard_map(
        body,
        mesh=mesh,
        in_specs=placed,
        out_specs=(P(("dp", "expert"), None), P(), P()),
        check_vma=False,
    )
```

```python
import functools

import jax
import jax.numpy as jnp
from jax import lax
from jax.experimental import pallas as pl
from jax.experimental.pallas import tpu as pltpu
from jax.sharding import PartitionSpec as P

bias_rate = 0.05
MESH = pl.DeviceIdType.MESH
VMEM_BYTES = 67043328
chunks = 16
lane_count = 128
copies = 8
crossed = (3, 6)
straight_chunks = 1


def expert_products(received, gate_w, up_w, down_w):
    gate_act = jnp.einsum("sjcd,jfd->sjcf", received, gate_w, preferred_element_type=jnp.float32)
    up_act = jnp.einsum("sjcd,jfd->sjcf", received, up_w, preferred_element_type=jnp.float32)
    hidden = (jax.nn.silu(gate_act) * up_act).astype(jnp.bfloat16)
    return jnp.einsum("sjcf,jfd->sjcd", hidden, down_w, preferred_element_type=jnp.float32)


def exchange_body(tokens, routes, route_weight, bias, w_gate, w_up, w_down):
    tok_rows, feature_width = tokens.shape
    top_count = routes.shape[1]
    experts = bias.shape[0]
    groups = lax.axis_size("expert")
    per_device = w_gate.shape[0]
    capacity = 5 * tok_rows * top_count // (4 * experts)
    flat_routes = routes.reshape(-1)
    labels = jnp.arange(experts, dtype=jnp.int32)
    picked = (flat_routes[:, None] == labels[None, :]).astype(jnp.int32)
    running = jnp.cumsum(picked, axis=0) - picked
    slot_rank = jnp.sum(running * picked, axis=1)
    local_counts = jnp.sum(picked, axis=0)
    kept_mask = slot_rank < capacity
    slot_total = experts * capacity
    slot_index = jnp.where(kept_mask, flat_routes * capacity + slot_rank, slot_total)
    token_index = jnp.arange(tok_rows * top_count, dtype=jnp.int32) // top_count
    source = jnp.zeros((slot_total + 1,), jnp.int32).at[slot_index].set(token_index)[:slot_total]
    filled = jnp.zeros((slot_total + 1,), jnp.bool_).at[slot_index].set(True)[:slot_total]
    send_rows = jnp.where(filled[:, None], tokens[source], jnp.zeros((), jnp.bfloat16))
    send_rows = send_rows.reshape(groups, per_device, capacity, feature_width)
    gathered = [lax.all_gather(w, "dp", axis=1, tiled=True) for w in (w_gate, w_up, w_down)]
    produced = expert_products(
        lax.all_to_all(send_rows, "expert", split_axis=0, concat_axis=0, tiled=True), *gathered
    ).astype(jnp.bfloat16)
    returned = lax.all_to_all(produced, "expert", split_axis=0, concat_axis=0, tiled=True)
    flat_out = returned.reshape(slot_total, feature_width)
    fetched = flat_out[jnp.minimum(slot_index, slot_total - 1)]
    entry_weight = jnp.where(kept_mask, route_weight.reshape(-1), jnp.float32(0.0))
    weighted = fetched.astype(jnp.float32) * entry_weight[:, None]
    mixed = jnp.sum(weighted.reshape(tok_rows, top_count, feature_width), axis=1).astype(
        jnp.bfloat16
    )
    mean_load = tok_rows * top_count * lax.axis_size("dp") * groups
    totals = lax.psum(local_counts.astype(jnp.float32), ("dp", "expert"))
    new_bias = bias + bias_rate * jnp.sign(mean_load - experts * totals)
    return (mixed, new_bias, totals.astype(jnp.int32))


def layer_kernel(
    zs, capacity, per_device, load,
    tokens, routes_any, weights_any, bias_any, w_gate, w_up, w_down,
    out, new_bias, counts,
    routes_t, weights_t, bias, tok, table, gate_w, up_w, down_w, scale, hidden, held,
    part1, keep1, recv1, part2, keep2, recv2, far2, mix2,
    keep3, part3, recv3, far3, own3, mix3, part4, recv4, early, tally, tally_in,
    own_sem, own_d, tok_in, tok_out, tab_in, tab_out, w_in, w_out, d_in, d_out,
    m_in, m_out, md_in, md_out, f_in, f_out, fd_in, fd_out,
    s1_in, s1_out, s2_in, s2_out, c2_in, s3_in, s3_out, c3_in, s4_in, s4_out,
    s5_in, t_in, t_out, turn,
):
    rows, width = tokens.shape
    top = routes_t.shape[0]
    experts = table.shape[1] // 2
    pieces, lanes, _ = w_gate.shape
    ff = pieces * lanes
    unit = ff // per_device
    cd = width // chunks
    slots = tok.shape[0]
    dp, ex = lax.axis_index("dp"), lax.axis_index("expert")
    y, x = dp // 2, dp % 2
    z, c = ex // 2, ex % 2

    def at(y_, x_, z_, c_):
        return (y_ * 2 + x_, z_ * 2 + c_)

    def slot(y_, z_):
        return y_ * zs + z_

    def far(step):
        return lax.rem(z + step, zs)

    mate = at(y, x, z, 1 - c)
    y_side = at(1 - y, x, z, c)
    x_side = at(y, 1 - x, z, c)
    x_mate = at(y, 1 - x, z, 1 - c)
    me = slot(y, z)

    barrier = pltpu.get_barrier_semaphore()
    partners = [mate, y_side, x_side, x_mate] + [at(y, x, far(s), c) for s in range(1, zs)]
    for partner in partners:
        pl.semaphore_signal(barrier, inc=1, device_id=partner, device_id_type=MESH)

    def span(j):
        return pl.ds(pl.multiple_of(j * cd, cd), cd)

    own = [
        pltpu.make_async_copy(tokens, tok.at[me], own_sem.at[0]),
        pltpu.make_async_copy(w_gate, gate_w.at[0, :, 0], own_sem.at[1]),
        pltpu.make_async_copy(w_up, up_w.at[0, :, 0], own_sem.at[2]),
        pltpu.make_async_copy(routes_any, routes_t, own_sem.at[3]),
        pltpu.make_async_copy(weights_any, weights_t, own_sem.at[4]),
        pltpu.make_async_copy(bias_any, bias, own_sem.at[5]),
    ]
    for copy in own:
        copy.start()

    def own_down(j):
        return pltpu.make_async_copy(w_down.at[:, :, span(j)], down_w.at[j, 0, :, 0], own_d)

    pl.semaphore_wait(barrier, len(partners))

    def remote(src, dst, ssem, rsem, device):
        copy = pltpu.make_async_remote_copy(
            src_ref=src, dst_ref=dst, send_sem=ssem, recv_sem=rsem,
            device_id=device, device_id_type=MESH,
        )
        copy.start()
        return copy

    def landed(ref, sem):
        pltpu.make_async_copy(ref, ref, sem).wait()

    def cross(n, p, source, target):
        final = n == 1 and p == pieces - 1
        return remote(
            source.at[p], target.at[1, p, 0], w_out.at[1 if final else 0], w_in.at[n, p],
            x_side,
        )

    def cross_down(j):
        remote(
            w_down.at[:, :, span(j)], down_w.at[j, 1, :, 0], d_out, d_in.at[j], x_side
        )

    for p in range(pieces):
        cross(0, p, w_gate, gate_w)
        last_up = cross(1, p, w_up, up_w)
    cross_down(0)

    def pass_table(n, index, device):
        remote(table.at[index], table.at[index], tab_out.at[n], tab_in.at[index], device)

    def pass_tokens(n, index, device, source):
        remote(source, tok.at[index], tok_out.at[n], tok_in.at[index], device)

    def pass_on(n, index, device):
        pass_table(n, index, device)
        pass_tokens(n, index, device, tok.at[index])

    def passed(n, count):
        landed(table.at[pl.ds(0, count)], tab_out.at[n])
        landed(tok.at[pl.ds(0, count)], tok_out.at[n])

    def arrived(index):
        landed(table.at[index], tab_in.at[index])
        landed(tok.at[index], tok_in.at[index])

    above, below = z < zs - 1, z > 0
    z_up, z_down = at(y, x, z + 1, c), at(y, x, z - 1, c)

    @pl.when(above)
    def _():
        pass_tokens(0, me, z_up, tokens)

    @pl.when(below)
    def _():
        pass_tokens(0, me, z_down, tokens)

    pass_tokens(1, me, y_side, tokens)

    remote(w_gate, gate_w.at[0, :, 1], m_out, m_in.at[0], mate)
    remote(w_up, up_w.at[0, :, 1], m_out, m_in.at[1], mate)

    def spread(j, carry):
        own_down(j).start()
        remote(
            w_down.at[:, :, span(j)], down_w.at[j, 0, :, 1], md_out, md_in, mate
        )
        return carry

    lax.fori_loop(0, chunks, spread, 0)

    for copy in own[3:]:
        copy.wait()

    labels = lax.broadcasted_iota(jnp.int32, (experts, rows), 0)
    picked = jnp.zeros((experts, rows), jnp.float32)
    weight = jnp.zeros((experts, rows), jnp.float32)
    for k in range(top):
        same = labels == routes_t[k : k + 1, :]
        picked += jnp.where(same, 1.0, 0.0)
        weight += jnp.where(same, weights_t[k : k + 1, :], 0.0)
    earlier = jnp.where(
        lax.broadcasted_iota(jnp.int32, (rows, rows), 0)
        < lax.broadcasted_iota(jnp.int32, (rows, rows), 1),
        1.0,
        0.0,
    )
    rank = jnp.dot(
        picked.astype(jnp.bfloat16),
        earlier.astype(jnp.bfloat16),
        preferred_element_type=jnp.float32,
    )
    table[me, 0:experts, :] = jnp.where(rank < capacity, weight, 0.0)
    table[me, experts : 2 * experts, :] = picked

    @pl.when(above)
    def _():
        pass_table(0, me, z_up)

    @pl.when(below)
    def _():
        pass_table(0, me, z_down)

    pass_table(1, me, y_side)
    for copy in own[:3]:
        copy.wait()

    def relay(source, onward, device):
        index = slot(y, source)
        arrived(index)

        @pl.when(onward)
        def _():
            pass_on(0, index, device)

        pass_on(1, index, y_side)

    for d in range(1, zs):

        @pl.when(z >= d)
        def _():
            relay(z - d, above, z_up)

        @pl.when(z + d < zs)
        def _():
            relay(z + d, below, z_down)

    def forward(n, p, target):
        landed(target.at[1, p, 0], w_in.at[n, p])
        remote(target.at[1, p, 0], target.at[1, p, 1], f_out, f_in.at[n, p], mate)

    for p in range(pieces - 1):
        forward(0, p, gate_w)
        forward(1, p, up_w)

    def from_y(i, carry):
        arrived(slot(1 - y, i))
        return carry

    lax.fori_loop(0, zs, from_y, 0)

    def add_tally(i, total):
        return total + table[i, experts : 2 * experts, :]

    tally[...] = lax.fori_loop(0, slots, add_tally, jnp.zeros((experts, rows), jnp.float32))
    for i, device in enumerate((x_side, mate, x_mate)):
        remote(tally, tally_in.at[i], t_out, t_in.at[i], device)

    place = lax.broadcasted_iota(jnp.int32, (rows, lanes), 1)

    def fill(index, carry):
        for k in range(2):
            first = (z * 2 + (c if k == 0 else 1 - c)) * per_device
            columns = []
            for j in range(per_device):
                row = table[index, pl.ds(first + j, 1), :]
                columns.append(jnp.transpose(jnp.broadcast_to(row, (lanes, rows))))
            for p in range(pieces):
                piece = columns[0]
                for j in range(1, per_device):
                    piece = jnp.where(place + p * lanes >= j * unit, columns[j], piece)
                scale[p, index, :, k * lanes : (k + 1) * lanes] = piece
        return carry

    lax.fori_loop(0, slots, fill, 0)

    nt = (((1,), (1,)), ((), ()))
    pair = 2 * lanes

    def project(q, h, p, source):
        block = tok[pl.ds(q * zs, zs)].reshape(zs * rows, width)
        return lax.dot_general(
            block, source[h, p].reshape(pair, width), nt, preferred_element_type=jnp.float32
        )

    def gated(q, p, gate):
        value = gate / (1.0 + jnp.exp(-gate))
        factor = scale[p, pl.ds(q * zs, zs)].reshape(zs * rows, pair)
        return value * factor

    def activate(q, h, p, gate, up):
        first = (h * pieces + p) * pair
        value = (gate * up).astype(jnp.bfloat16)
        hidden[pl.ds(q * zs, zs), :, first : first + pair] = value.reshape(zs, rows, pair)

    def both(h, p):
        def step(q, carry):
            gate = gated(q, p, project(q, h, p, gate_w))
            activate(q, h, p, gate, project(q, h, p, up_w))
            return carry

        lax.fori_loop(0, 2, step, 0)

    landed(gate_w.at[0, :, 1], m_in.at[0])
    landed(up_w.at[0, :, 1], m_in.at[1])
    for p in range(pieces):
        both(0, p)
    for p in range(pieces - 1):
        landed(gate_w.at[1, p, 1], f_in.at[0, p])
        landed(up_w.at[1, p, 1], f_in.at[1, p])
        both(1, p)

    last = pieces - 1
    forward(0, last, gate_w)
    landed(gate_w.at[1, last, 1], f_in.at[0, last])

    def hold(q, carry):
        held[q] = gated(q, last, project(q, 1, last, gate_w))
        return carry

    lax.fori_loop(0, 2, hold, 0)

    def fetch(j):
        landed(down_w.at[j, 1, :, 0], d_in.at[j])
        remote(
            down_w.at[j, 1, :, 0], down_w.at[j, 1, :, 1], fd_out, fd_in.at[j], mate
        )

    def ready(j):
        landed(down_w.at[j, 1, :, 1], fd_in.at[j])

    landed(down_w.at[:, 0, :, 0], own_d)
    landed(down_w.at[:, 0, :, 1], md_in)
    known = 2 * ff

    def begin(q, carry):
        near = hidden[pl.ds(q * zs, zs), :, 0:known].reshape(zs * rows, known)
        weights = down_w[0, 0].reshape(known, cd)
        early[q] = jnp.dot(near, weights, preferred_element_type=jnp.float32)
        return carry

    lax.fori_loop(0, 2, begin, 0)

    last_up.wait_send()
    pl.semaphore_signal(turn, inc=1, device_id=mate, device_id_type=MESH)
    pl.semaphore_wait(turn, 1)

    def follow(j, carry):
        cross_down(j)
        return carry

    lax.fori_loop(1, chunks, follow, 0)
    forward(1, last, up_w)
    landed(up_w.at[1, last, 1], f_in.at[1, last])

    def finish(q):
        block = tok[pl.ds(q * zs, zs)].reshape(zs * rows, width)
        part = up_w[1, last].reshape(pair, width)
        half = width // 2
        ups = [
            lax.dot_general(
                block[:, k * half : (k + 1) * half], part[:, k * half : (k + 1) * half],
                nt, preferred_element_type=jnp.float32,
            )
            for k in range(2)
        ]
        first = (2 * pieces - 1) * pair
        value = (held[q] * ups[0] + held[q] * ups[1]).astype(jnp.bfloat16)
        hidden[pl.ds(q * zs, zs), :, first : first + pair] = value.reshape(zs, rows, pair)

    def down(q, j):
        near = hidden[pl.ds(q * zs, zs)].reshape(zs * rows, 4 * ff)
        return jnp.dot(
            near, down_w[j].reshape(4 * ff, cd), preferred_element_type=jnp.float32
        ).reshape(zs, rows, cd)

    def down_first(q):
        near = hidden[pl.ds(q * zs, zs), :, known : 4 * ff].reshape(zs * rows, known)
        weights = down_w[0, 1].reshape(known, cd)
        value = early[q] + jnp.dot(near, weights, preferred_element_type=jnp.float32)
        return value.reshape(zs, rows, cd)

    end = jnp.logical_or(z == 0, z == zs - 1)
    inner = jnp.logical_not(end)
    beside = z + 1 - 2 * lax.rem(z, 2)
    across = lax.rem(z + 2, zs)
    mirror = zs - 1 - z
    straight = jnp.where(end, across, mirror)
    longest = jnp.where(end, mirror, across)
    order = (longest, straight, beside, z)
    final = chunks - 1

    def away(j, value):
        part1[j] = value.astype(jnp.bfloat16)

        @pl.when(j < final)
        def _():
            remote(part1.at[j], recv1.at[j], s1_out, s1_in.at[j], y_side)

        @pl.when(j == final)
        def _():
            for i, n in enumerate(order):
                remote(part1.at[j, n], recv1.at[j, n], s1_out, s5_in.at[i], y_side)

    lane = jnp.where(end, 1, 2)

    def out_z(j, value, part, recv, kept, mix, outs, ins, mix_in, direct=None):
        def send(i, n, target, sem, device):
            part[j, i] = value(n).astype(jnp.bfloat16)
            remote(part.at[j, i], target, outs, sem, at(y, x, device, c))

        def relayed():
            @pl.when(end)
            def _():
                send(2, mirror, mix.at[j], mix_in.at[j], beside)

            @pl.when(inner)
            def _():
                kept[j] = value(across)

        def unrelayed():
            @pl.when(end)
            def _():
                send(2, mirror, recv.at[j, 2], ins.at[j], mirror)

            @pl.when(inner)
            def _():
                send(2, across, recv.at[j, 1], ins.at[j], across)

        if direct is None:
            relayed()
        else:
            pl.when(direct)(unrelayed)
            pl.when(jnp.logical_not(direct))(relayed)

        send(1, straight, recv.at[j, lane], ins.at[j], straight)
        send(0, beside, recv.at[j, 0], ins.at[j], beside)

    def merge(j, part, recv, kept, mix, outs, ins, mix_in):
        @pl.when(inner)
        def _():
            landed(mix.at[j], mix_in.at[j])
            part[j, 2] = (kept[j] + mix[j].astype(jnp.float32)).astype(jnp.bfloat16)
            remote(
                part.at[j, 2], recv.at[j, 1], outs, ins.at[j],
                at(y, x, across, c),
            )

    def in_z(j, total, recv, ins, third):
        def add(count):
            landed(recv.at[j, pl.ds(0, count)], ins.at[j])
            value = total[j]
            for i in range(count):
                value = value + recv[j, i].astype(jnp.float32)
            total[j] = value

        pl.when(third)(lambda: add(3))
        pl.when(jnp.logical_not(third))(lambda: add(2))

    def is_last(j):
        return j >= chunks - straight_chunks

    def last_y(j):
        def value(n):
            return keep1[j, n] + recv1[j, n].astype(jnp.float32)

        targets = (jnp.where(end, 2, 1), lane, 0)
        for i, n in enumerate(order):
            landed(recv1.at[j, n], s5_in.at[i])
            if i < zs - 1:
                part2[j, i] = value(n).astype(jnp.bfloat16)
                remote(
                    part2.at[j, i], recv2.at[j, targets[i]], s2_out, s2_in.at[j],
                    at(y, x, n, c),
                )
        keep2[j] = value(z)

    def over_y(j):
        landed(recv1.at[j], s1_in.at[j])

        def value(n):
            return keep1[j, n] + recv1[j, n].astype(jnp.float32)

        out_z(j, value, part2, recv2, far2, mix2, s2_out, s2_in, c2_in, is_last(j))
        keep2[j] = value(z)

    def merge_y(j):
        merge(j, part2, recv2, far2, mix2, s2_out, s2_in, c2_in)

    def over_z(j):
        in_z(j, keep2, recv2, s2_in, jnp.logical_or(inner, is_last(j)))
        out[:, span(j)] = keep2[j].astype(jnp.bfloat16)

    def first_z(b):
        def value(n):
            return keep3[b, :, n]

        out_z(b, value, part3, recv3, far3, mix3, s3_out, s3_in, c3_in)
        own3[b] = value(z)

    def then_y(b):
        in_z(b, own3, recv3, s3_in, inner)
        part4[b] = own3[b, 1 - y].astype(jnp.bfloat16)
        remote(part4.at[b], recv4.at[b], s4_out, s4_in.at[b], y_side)

    def crossed_out(b, j):
        landed(recv4.at[b], s4_in.at[b])
        value = own3[b, y] + recv4[b].astype(jnp.float32)
        out[:, span(j)] = value.astype(jnp.bfloat16)

    finish(1 - y)
    fetch(0)
    ready(0)
    away(0, down_first(1 - y))
    finish(y)
    fetch(1)
    keep1[0] = down_first(y)

    def tell():
        count = tally[...]
        for i in range(3):
            landed(tally_in.at[i], t_in.at[i])
            count += tally_in[i]
        row = lax.dot_general(
            jnp.ones((8, rows), jnp.bfloat16), count.astype(jnp.bfloat16), nt,
            preferred_element_type=jnp.float32,
        )[0:1]
        spare = load - experts * row
        change = jnp.where(spare > 0.0, bias_rate, jnp.where(spare < 0.0, -bias_rate, 0.0))
        new_bias[...] = bias[...] + change
        counts[...] = row.astype(jnp.int32)

    lag_y, lag_m, lag_z = 2, 5, 10
    late = chunks - straight_chunks - 3

    def plain(j):
        ok = jnp.logical_and(j >= 0, j < chunks)
        for special in crossed:
            ok = jnp.logical_and(ok, j != special)
        return ok

    def step(j, carry):
        @pl.when(j < chunks)
        def _():
            ready(j)

            @pl.when(plain(j))
            def _():
                away(j, down(1 - y, j))

            for b, special in enumerate(crossed):

                @pl.when(j == special)
                def _(b=b):
                    keep3[b, 1 - y] = down(1 - y, j)

            @pl.when(j < chunks - 1)
            def _():
                fetch(j + 1)

            @pl.when(plain(j))
            def _():
                keep1[j] = down(y, j)

            for b, special in enumerate(crossed):

                @pl.when(j == special)
                def _(b=b):
                    keep3[b, y] = down(y, j)
                    first_z(b)

        pl.when(j == chunks)(tell)

        for lag, first, past in (
            (lag_m, 0, late), (lag_m - 1, late, chunks - straight_chunks)
        ):
            due = jnp.logical_and(j - lag >= first, j - lag < past)

            @pl.when(jnp.logical_and(plain(j - lag), due))
            def _(lag=lag):
                merge_y(j - lag)

        @pl.when(jnp.logical_and(plain(j - lag_y), j - lag_y < final))
        def _():
            over_y(j - lag_y)

        @pl.when(j - lag_y == final)
        def _():
            last_y(final)

        for b, special in enumerate(crossed):

            @pl.when(j == special + 5)
            def _(b=b):
                merge(b, part3, recv3, far3, mix3, s3_out, s3_in, c3_in)

            @pl.when(j == special + 8)
            def _(b=b):
                then_y(b)

            @pl.when(j == special + 11)
            def _(b=b, special=special):
                crossed_out(b, special)

        @pl.when(plain(j - lag_z))
        def _():
            over_z(j - lag_z)

        return carry

    lax.fori_loop(1, chunks + lag_z, step, 0)

    landed(gate_w.at[:, :, 1], m_out)
    landed(gate_w.at[:, :, 1], f_out)
    landed(tok.at[pl.ds(0, 2 * pieces - 1)], w_out.at[0])
    landed(tally_in, t_out)

    for sem in (d_out, md_out, fd_out):
        landed(down_w.at[:, 1, :, 0], sem)
    usual = pl.ds(0, chunks - len(crossed))
    landed(part1.at[usual], s1_out)
    landed(part2.at[usual], s2_out)
    landed(part3, s3_out)
    landed(part4, s4_out)

    passed(1, zs)

    @pl.when(end)
    def _():
        passed(0, 1)

    @pl.when(inner)
    def _():
        passed(0, zs + 1)


def group_scratch(zs, rows, top, width, ff, experts):
    slots = 2 * zs
    cd = width // chunks
    pieces = ff // lane_count
    twice = len(crossed)
    bf, f32 = jnp.bfloat16, jnp.float32
    return [
        ((top, rows), jnp.int32),
        ((top, rows), f32),
        ((1, experts), f32),
        ((slots, rows, width), bf),
        ((slots, 2 * experts, rows), f32),
        ((2, pieces, 2, lane_count, width), bf),
        ((2, pieces, 2, lane_count, width), bf),
        ((chunks, 2, pieces, 2, lane_count, cd), bf),
        ((pieces, slots, rows, 2 * lane_count), f32),
        ((slots, rows, 4 * ff), bf),
        ((2, zs * rows, 2 * lane_count), f32),
        ((chunks, zs, rows, cd), bf),
        ((chunks, zs, rows, cd), f32),
        ((chunks, zs, rows, cd), bf),
        ((chunks, zs - 1, rows, cd), bf),
        ((chunks, rows, cd), f32),
        ((chunks, zs - 1, rows, cd), bf),
        ((chunks, rows, cd), f32),
        ((chunks, rows, cd), bf),
        ((twice, 2, zs, rows, cd), f32),
        ((twice, zs - 1, 2, rows, cd), bf),
        ((twice, zs - 1, 2, rows, cd), bf),
        ((twice, 2, rows, cd), f32),
        ((twice, 2, rows, cd), f32),
        ((twice, 2, rows, cd), bf),
        ((twice, rows, cd), bf),
        ((twice, rows, cd), bf),
        ((2, zs * rows, cd), f32),
        ((experts, rows), f32),
        ((3, experts, rows), f32),
    ]


def finish_kernel(mixed, new_bias, counts, mixed_out, bias_out, counts_out, done):
    rows = mixed.shape[0] // copies
    moves = [
        (mixed.at[pl.ds(i * rows, rows)], mixed_out.at[pl.ds(i * rows, rows)])
        for i in range(copies)
    ]
    moves += [(new_bias, bias_out), (counts, counts_out)]
    moves = [pltpu.make_async_copy(a, b, done.at[i]) for i, (a, b) in enumerate(moves)]
    for move in moves:
        move.start()
    for move in moves:
        move.wait()


def group_body(zs, tokens, routes, route_weight, bias, w_gate, w_up, w_down):
    rows, width = tokens.shape
    experts = bias.shape[0]
    per_device, unit, _ = w_gate.shape
    ff = per_device * unit
    top = routes.shape[1]
    capacity = 5 * rows * top // (4 * experts)
    slots = 2 * zs
    pieces = ff // lane_count
    twice = len(crossed)
    dma = pltpu.SemaphoreType.DMA
    vmem = pl.BlockSpec(memory_space=pltpu.VMEM)
    anywhere = pl.BlockSpec(memory_space=pl.ANY)
    split = (pieces, lane_count, width)
    mean_load = rows * top * lax.axis_size("dp") * lax.axis_size("expert")
    results = pl.pallas_call(
        functools.partial(layer_kernel, zs, capacity, per_device, mean_load),
        out_shape=(
            pltpu.VMEM((rows, width), jnp.bfloat16),
            pltpu.VMEM((1, experts), jnp.float32),
            pltpu.VMEM((1, experts), jnp.int32),
        ),
        in_specs=[anywhere] * 7,
        out_specs=(vmem, vmem, vmem),
        scratch_shapes=[
            pltpu.VMEM(shape, kind)
            for shape, kind in group_scratch(zs, rows, top, width, ff, experts)
        ]
        + [
            dma((6,)), dma, dma((slots,)), dma((2,)), dma((slots,)), dma((2,)),
            dma((2, pieces)), dma((2,)), dma((chunks,)), dma, dma((2,)), dma, dma, dma,
            dma((2, pieces)), dma, dma((chunks,)), dma,
            dma((chunks,)), dma, dma((chunks,)), dma, dma((chunks,)),
            dma((twice,)), dma, dma((twice,)), dma((twice,)), dma,
            dma((zs,)), dma((3,)), dma, pltpu.SemaphoreType.REGULAR,
        ],
        compiler_params=pltpu.CompilerParams(
            collective_id=0, has_side_effects=True, vmem_limit_bytes=60000000
        ),
    )(
        tokens, routes.T, route_weight.T, bias.reshape(1, experts),
        w_gate.reshape(split), w_up.reshape(split), w_down.reshape(split),
    )
    results = [pltpu.with_memory_space_constraint(a, pltpu.VMEM) for a in results]
    mixed, new_bias, counts = pl.pallas_call(
        finish_kernel,
        out_shape=(
            jax.ShapeDtypeStruct((rows, width), jnp.bfloat16),
            jax.ShapeDtypeStruct((1, experts), jnp.float32),
            jax.ShapeDtypeStruct((1, experts), jnp.int32),
        ),
        in_specs=[vmem, vmem, vmem],
        out_specs=(anywhere, anywhere, anywhere),
        scratch_shapes=[dma((copies + 2,))],
    )(*results)
    return (mixed, new_bias.reshape(experts), counts.reshape(experts))


def body(tokens, routes, route_weight, bias, w_gate, w_up, w_down):
    rows, width = tokens.shape
    per_device, unit, _ = w_gate.shape
    ff = per_device * unit
    groups = lax.axis_size("expert")
    zs = groups // 2
    held = group_scratch(zs, rows, routes.shape[1], width, ff, bias.shape[0])
    total = 0
    for shape, kind in held:
        size = jnp.dtype(kind).itemsize
        for extent in shape:
            size *= extent
        total += size
    args = (tokens, routes, route_weight, bias, w_gate, w_up, w_down)
    fits = total < 0.85 * VMEM_BYTES and rows == lane_count
    even = ff % lane_count == 0 and width % (chunks * lane_count) == 0
    if lax.axis_size("dp") == 4 and groups % 2 == 0 and zs == 4 and fits and even:
        return group_body(zs, *args)
    return exchange_body(*args)


def solution(mesh):
    placed = (
        P(("dp", "expert"), None),
        P(("dp", "expert"), None),
        P(("dp", "expert"), None),
        P(),
        P("expert", "dp", None),
        P("expert", "dp", None),
        P("expert", "dp", None),
    )
    return jax.shard_map(
        body,
        mesh=mesh,
        in_specs=placed,
        out_specs=(P(("dp", "expert"), None), P(), P()),
        check_vma=False,
    )
```

```python
import functools

import jax
import jax.numpy as jnp
from jax import lax
from jax.experimental import pallas as pl
from jax.experimental.pallas import tpu as pltpu
from jax.sharding import PartitionSpec as P

bias_rate = 0.05
MESH = pl.DeviceIdType.MESH
VMEM_BYTES = 67043328
chunks = 16
lane_count = 128
copies = 4
crossed = (3, 6)
straight_chunks = 1


def expert_products(received, gate_w, up_w, down_w):
    gate_act = jnp.einsum("sjcd,jfd->sjcf", received, gate_w, preferred_element_type=jnp.float32)
    up_act = jnp.einsum("sjcd,jfd->sjcf", received, up_w, preferred_element_type=jnp.float32)
    hidden = (jax.nn.silu(gate_act) * up_act).astype(jnp.bfloat16)
    return jnp.einsum("sjcf,jfd->sjcd", hidden, down_w, preferred_element_type=jnp.float32)


def exchange_body(tokens, routes, route_weight, bias, w_gate, w_up, w_down):
    tok_rows, feature_width = tokens.shape
    top_count = routes.shape[1]
    experts = bias.shape[0]
    groups = lax.axis_size("expert")
    per_device = w_gate.shape[0]
    capacity = 5 * tok_rows * top_count // (4 * experts)
    flat_routes = routes.reshape(-1)
    labels = jnp.arange(experts, dtype=jnp.int32)
    picked = (flat_routes[:, None] == labels[None, :]).astype(jnp.int32)
    running = jnp.cumsum(picked, axis=0) - picked
    slot_rank = jnp.sum(running * picked, axis=1)
    local_counts = jnp.sum(picked, axis=0)
    kept_mask = slot_rank < capacity
    slot_total = experts * capacity
    slot_index = jnp.where(kept_mask, flat_routes * capacity + slot_rank, slot_total)
    token_index = jnp.arange(tok_rows * top_count, dtype=jnp.int32) // top_count
    source = jnp.zeros((slot_total + 1,), jnp.int32).at[slot_index].set(token_index)[:slot_total]
    filled = jnp.zeros((slot_total + 1,), jnp.bool_).at[slot_index].set(True)[:slot_total]
    send_rows = jnp.where(filled[:, None], tokens[source], jnp.zeros((), jnp.bfloat16))
    send_rows = send_rows.reshape(groups, per_device, capacity, feature_width)
    gathered = [lax.all_gather(w, "dp", axis=1, tiled=True) for w in (w_gate, w_up, w_down)]
    produced = expert_products(
        lax.all_to_all(send_rows, "expert", split_axis=0, concat_axis=0, tiled=True), *gathered
    ).astype(jnp.bfloat16)
    returned = lax.all_to_all(produced, "expert", split_axis=0, concat_axis=0, tiled=True)
    flat_out = returned.reshape(slot_total, feature_width)
    fetched = flat_out[jnp.minimum(slot_index, slot_total - 1)]
    entry_weight = jnp.where(kept_mask, route_weight.reshape(-1), jnp.float32(0.0))
    weighted = fetched.astype(jnp.float32) * entry_weight[:, None]
    mixed = jnp.sum(weighted.reshape(tok_rows, top_count, feature_width), axis=1).astype(
        jnp.bfloat16
    )
    mean_load = tok_rows * top_count * lax.axis_size("dp") * groups
    totals = lax.psum(local_counts.astype(jnp.float32), ("dp", "expert"))
    new_bias = bias + bias_rate * jnp.sign(mean_load - experts * totals)
    return (mixed, new_bias, totals.astype(jnp.int32))


def layer_kernel(
    zs, capacity, per_device, load,
    tokens, routes_any, weights_any, bias_any, w_gate, w_up, w_down,
    out, new_bias, counts,
    routes_t, weights_t, bias, tok, table, gate_w, up_w, down_w, scale, hidden, held,
    part1, keep1, recv1, part2, keep2, recv2, far2, mix2,
    keep3, part3, recv3, far3, own3, mix3, part4, recv4, early, tally, tally_in,
    own_sem, own_d, tok_in, tok_out, tab_in, tab_out, w_in, w_out, d_in, d_out,
    m_in, m_out, md_in, md_out, f_in, f_out, fd_in, fd_out,
    s1_in, s1_out, s2_in, s2_out, c2_in, s3_in, s3_out, c3_in, s4_in, s4_out,
    s5_in, t_in, t_out, turn,
):
    rows, width = tokens.shape
    top = routes_t.shape[0]
    experts = table.shape[1] // 2
    pieces, lanes, _ = w_gate.shape
    ff = pieces * lanes
    unit = ff // per_device
    cd = width // chunks
    slots = tok.shape[0]
    dp, ex = lax.axis_index("dp"), lax.axis_index("expert")
    y, x = dp // 2, dp % 2
    z, c = ex // 2, ex % 2

    def at(y_, x_, z_, c_):
        return (y_ * 2 + x_, z_ * 2 + c_)

    def slot(y_, z_):
        return y_ * zs + z_

    def far(step):
        return lax.rem(z + step, zs)

    mate = at(y, x, z, 1 - c)
    y_side = at(1 - y, x, z, c)
    x_side = at(y, 1 - x, z, c)
    x_mate = at(y, 1 - x, z, 1 - c)
    me = slot(y, z)

    barrier = pltpu.get_barrier_semaphore()
    partners = [mate, y_side, x_side, x_mate] + [at(y, x, far(s), c) for s in range(1, zs)]
    for partner in partners:
        pl.semaphore_signal(barrier, inc=1, device_id=partner, device_id_type=MESH)

    def span(j):
        return pl.ds(pl.multiple_of(j * cd, cd), cd)

    own = [
        pltpu.make_async_copy(tokens, tok.at[me], own_sem.at[0]),
        pltpu.make_async_copy(w_gate, gate_w.at[0, :, 0], own_sem.at[1]),
        pltpu.make_async_copy(w_up, up_w.at[0, :, 0], own_sem.at[2]),
        pltpu.make_async_copy(routes_any, routes_t, own_sem.at[3]),
        pltpu.make_async_copy(weights_any, weights_t, own_sem.at[4]),
        pltpu.make_async_copy(bias_any, bias, own_sem.at[5]),
    ]
    for copy in own:
        copy.start()

    def own_down(j):
        return pltpu.make_async_copy(w_down.at[:, :, span(j)], down_w.at[j, 0, :, 0], own_d)

    pl.semaphore_wait(barrier, len(partners))

    def remote(src, dst, ssem, rsem, device):
        copy = pltpu.make_async_remote_copy(
            src_ref=src, dst_ref=dst, send_sem=ssem, recv_sem=rsem,
            device_id=device, device_id_type=MESH,
        )
        copy.start()
        return copy

    def landed(ref, sem):
        pltpu.make_async_copy(ref, ref, sem).wait()

    def cross(n, p, source, target):
        final = n == 1 and p == pieces - 1
        return remote(
            source.at[p], target.at[1, p, 0], w_out.at[1 if final else 0], w_in.at[n, p],
            x_side,
        )

    def cross_down(j):
        remote(
            w_down.at[:, :, span(j)], down_w.at[j, 1, :, 0], d_out, d_in.at[j], x_side
        )

    for p in range(pieces):
        cross(0, p, w_gate, gate_w)
        last_up = cross(1, p, w_up, up_w)
    cross_down(0)

    def pass_table(n, index, device):
        remote(table.at[index], table.at[index], tab_out.at[n], tab_in.at[index], device)

    def pass_tokens(n, index, device, source):
        remote(source, tok.at[index], tok_out.at[n], tok_in.at[index], device)

    def pass_on(n, index, device):
        pass_table(n, index, device)
        pass_tokens(n, index, device, tok.at[index])

    def passed(n, count):
        landed(table.at[pl.ds(0, count)], tab_out.at[n])
        landed(tok.at[pl.ds(0, count)], tok_out.at[n])

    def arrived(index):
        landed(table.at[index], tab_in.at[index])
        landed(tok.at[index], tok_in.at[index])

    above, below = z < zs - 1, z > 0
    z_up, z_down = at(y, x, z + 1, c), at(y, x, z - 1, c)

    @pl.when(above)
    def _():
        pass_tokens(0, me, z_up, tokens)

    @pl.when(below)
    def _():
        pass_tokens(0, me, z_down, tokens)

    pass_tokens(1, me, y_side, tokens)

    remote(w_gate, gate_w.at[0, :, 1], m_out, m_in.at[0], mate)
    remote(w_up, up_w.at[0, :, 1], m_out, m_in.at[1], mate)

    def spread(j, carry):
        own_down(j).start()
        remote(
            w_down.at[:, :, span(j)], down_w.at[j, 0, :, 1], md_out, md_in, mate
        )
        return carry

    lax.fori_loop(0, chunks, spread, 0)

    for copy in own[3:]:
        copy.wait()

    labels = lax.broadcasted_iota(jnp.int32, (experts, rows), 0)
    picked = jnp.zeros((experts, rows), jnp.float32)
    weight = jnp.zeros((experts, rows), jnp.float32)
    for k in range(top):
        same = labels == routes_t[k : k + 1, :]
        picked += jnp.where(same, 1.0, 0.0)
        weight += jnp.where(same, weights_t[k : k + 1, :], 0.0)
    earlier = jnp.where(
        lax.broadcasted_iota(jnp.int32, (rows, rows), 0)
        < lax.broadcasted_iota(jnp.int32, (rows, rows), 1),
        1.0,
        0.0,
    )
    rank = jnp.dot(
        picked.astype(jnp.bfloat16),
        earlier.astype(jnp.bfloat16),
        preferred_element_type=jnp.float32,
    )
    table[me, 0:experts, :] = jnp.where(rank < capacity, weight, 0.0)
    table[me, experts : 2 * experts, :] = picked

    @pl.when(above)
    def _():
        pass_table(0, me, z_up)

    @pl.when(below)
    def _():
        pass_table(0, me, z_down)

    pass_table(1, me, y_side)
    for copy in own[:3]:
        copy.wait()

    def relay(source, onward, device):
        index = slot(y, source)
        arrived(index)

        @pl.when(onward)
        def _():
            pass_on(0, index, device)

        pass_on(1, index, y_side)

    for d in range(1, zs):

        @pl.when(z >= d)
        def _():
            relay(z - d, above, z_up)

        @pl.when(z + d < zs)
        def _():
            relay(z + d, below, z_down)

    def forward(n, p, target):
        landed(target.at[1, p, 0], w_in.at[n, p])
        remote(target.at[1, p, 0], target.at[1, p, 1], f_out, f_in.at[n, p], mate)

    for p in range(pieces - 1):
        forward(0, p, gate_w)
        forward(1, p, up_w)

    def from_y(i, carry):
        arrived(slot(1 - y, i))
        return carry

    lax.fori_loop(0, zs, from_y, 0)

    def add_tally(i, total):
        return total + table[i, experts : 2 * experts, :]

    tally[...] = lax.fori_loop(0, slots, add_tally, jnp.zeros((experts, rows), jnp.float32))
    for i, device in enumerate((x_side, mate, x_mate)):
        remote(tally, tally_in.at[i], t_out, t_in.at[i], device)

    place = lax.broadcasted_iota(jnp.int32, (rows, lanes), 1)

    def fill(index, carry):
        for k in range(2):
            first = (z * 2 + (c if k == 0 else 1 - c)) * per_device
            columns = []
            for j in range(per_device):
                row = table[index, pl.ds(first + j, 1), :]
                columns.append(jnp.transpose(jnp.broadcast_to(row, (lanes, rows))))
            for p in range(pieces):
                piece = columns[0]
                for j in range(1, per_device):
                    piece = jnp.where(place + p * lanes >= j * unit, columns[j], piece)
                scale[p, index, :, k * lanes : (k + 1) * lanes] = piece
        return carry

    lax.fori_loop(0, slots, fill, 0)

    nt = (((1,), (1,)), ((), ()))
    pair = 2 * lanes

    def project(q, h, p, source):
        block = tok[pl.ds(q * zs, zs)].reshape(zs * rows, width)
        return lax.dot_general(
            block, source[h, p].reshape(pair, width), nt, preferred_element_type=jnp.float32
        )

    def gated(q, p, gate):
        value = gate / (1.0 + jnp.exp(-gate))
        factor = scale[p, pl.ds(q * zs, zs)].reshape(zs * rows, pair)
        return value * factor

    def activate(q, h, p, gate, up):
        first = (h * pieces + p) * pair
        value = (gate * up).astype(jnp.bfloat16)
        hidden[pl.ds(q * zs, zs), :, first : first + pair] = value.reshape(zs, rows, pair)

    def both(h, p):
        def step(q, carry):
            gate = gated(q, p, project(q, h, p, gate_w))
            activate(q, h, p, gate, project(q, h, p, up_w))
            return carry

        lax.fori_loop(0, 2, step, 0)

    landed(gate_w.at[0, :, 1], m_in.at[0])
    landed(up_w.at[0, :, 1], m_in.at[1])
    for p in range(pieces):
        both(0, p)
    for p in range(pieces - 1):
        landed(gate_w.at[1, p, 1], f_in.at[0, p])
        landed(up_w.at[1, p, 1], f_in.at[1, p])
        both(1, p)

    last = pieces - 1
    forward(0, last, gate_w)
    landed(gate_w.at[1, last, 1], f_in.at[0, last])

    def hold(q, carry):
        held[q] = gated(q, last, project(q, 1, last, gate_w))
        return carry

    lax.fori_loop(0, 2, hold, 0)

    def fetch(j):
        landed(down_w.at[j, 1, :, 0], d_in.at[j])
        remote(
            down_w.at[j, 1, :, 0], down_w.at[j, 1, :, 1], fd_out, fd_in.at[j], mate
        )

    def ready(j):
        landed(down_w.at[j, 1, :, 1], fd_in.at[j])

    landed(down_w.at[:, 0, :, 0], own_d)
    landed(down_w.at[:, 0, :, 1], md_in)
    known = 2 * ff

    last_up.wait_send()
    pl.semaphore_signal(turn, inc=1, device_id=mate, device_id_type=MESH)
    pl.semaphore_wait(turn, 1)

    def follow(j, carry):
        cross_down(j)
        return carry

    lax.fori_loop(1, chunks, follow, 0)
    def begin(q, carry):
        near = hidden[pl.ds(q * zs, zs), :, 0:known].reshape(zs * rows, known)
        weights = down_w[0, 0].reshape(known, cd)
        early[q] = jnp.dot(near, weights, preferred_element_type=jnp.float32)
        return carry

    lax.fori_loop(0, 2, begin, 0)

    forward(1, last, up_w)
    landed(up_w.at[1, last, 1], f_in.at[1, last])

    def finish(q):
        block = tok[pl.ds(q * zs, zs)].reshape(zs * rows, width)
        part = up_w[1, last].reshape(pair, width)
        half = width // 2
        ups = [
            lax.dot_general(
                block[:, k * half : (k + 1) * half], part[:, k * half : (k + 1) * half],
                nt, preferred_element_type=jnp.float32,
            )
            for k in range(2)
        ]
        first = (2 * pieces - 1) * pair
        value = (held[q] * ups[0] + held[q] * ups[1]).astype(jnp.bfloat16)
        hidden[pl.ds(q * zs, zs), :, first : first + pair] = value.reshape(zs, rows, pair)

    def down(q, j):
        near = hidden[pl.ds(q * zs, zs)].reshape(zs * rows, 4 * ff)
        return jnp.dot(
            near, down_w[j].reshape(4 * ff, cd), preferred_element_type=jnp.float32
        ).reshape(zs, rows, cd)

    def down_first(q):
        near = hidden[pl.ds(q * zs, zs), :, known : 4 * ff].reshape(zs * rows, known)
        weights = down_w[0, 1].reshape(known, cd)
        value = early[q] + jnp.dot(near, weights, preferred_element_type=jnp.float32)
        return value.reshape(zs, rows, cd)

    end = jnp.logical_or(z == 0, z == zs - 1)
    inner = jnp.logical_not(end)
    beside = z + 1 - 2 * lax.rem(z, 2)
    across = lax.rem(z + 2, zs)
    mirror = zs - 1 - z
    straight = jnp.where(end, across, mirror)
    longest = jnp.where(end, mirror, across)
    order = (longest, straight, beside, z)
    final = chunks - 1

    def away(j, value):
        part1[j] = value.astype(jnp.bfloat16)

        @pl.when(j < final)
        def _():
            remote(part1.at[j], recv1.at[j], s1_out, s1_in.at[j], y_side)

        @pl.when(j == final)
        def _():
            for i, n in enumerate(order):
                remote(part1.at[j, n], recv1.at[j, n], s1_out, s5_in.at[i], y_side)

    lane = jnp.where(end, 1, 2)

    def out_z(j, value, part, recv, kept, mix, outs, ins, mix_in, direct=None):
        def send(i, n, target, sem, device):
            part[j, i] = value(n).astype(jnp.bfloat16)
            remote(part.at[j, i], target, outs, sem, at(y, x, device, c))

        def relayed():
            @pl.when(end)
            def _():
                send(2, mirror, mix.at[j], mix_in.at[j], beside)

            @pl.when(inner)
            def _():
                kept[j] = value(across)

        def unrelayed():
            @pl.when(end)
            def _():
                send(2, mirror, recv.at[j, 2], ins.at[j], mirror)

            @pl.when(inner)
            def _():
                send(2, across, recv.at[j, 1], ins.at[j], across)

        if direct is None:
            relayed()
        else:
            pl.when(direct)(unrelayed)
            pl.when(jnp.logical_not(direct))(relayed)

        send(1, straight, recv.at[j, lane], ins.at[j], straight)
        send(0, beside, recv.at[j, 0], ins.at[j], beside)

    def merge(j, part, recv, kept, mix, outs, ins, mix_in):
        @pl.when(inner)
        def _():
            landed(mix.at[j], mix_in.at[j])
            part[j, 2] = (kept[j] + mix[j].astype(jnp.float32)).astype(jnp.bfloat16)
            remote(
                part.at[j, 2], recv.at[j, 1], outs, ins.at[j],
                at(y, x, across, c),
            )

    def in_z(j, total, recv, ins, third):
        def add(count):
            landed(recv.at[j, pl.ds(0, count)], ins.at[j])
            value = total[j]
            for i in range(count):
                value = value + recv[j, i].astype(jnp.float32)
            total[j] = value

        pl.when(third)(lambda: add(3))
        pl.when(jnp.logical_not(third))(lambda: add(2))

    def is_last(j):
        return j >= chunks - straight_chunks

    def last_y(j):
        def value(n):
            return keep1[j, n] + recv1[j, n].astype(jnp.float32)

        targets = (jnp.where(end, 2, 1), lane, 0)
        for i, n in enumerate(order):
            landed(recv1.at[j, n], s5_in.at[i])
            if i < zs - 1:
                part2[j, i] = value(n).astype(jnp.bfloat16)
                remote(
                    part2.at[j, i], recv2.at[j, targets[i]], s2_out, s2_in.at[j],
                    at(y, x, n, c),
                )
        keep2[j] = value(z)

    def over_y(j):
        landed(recv1.at[j], s1_in.at[j])

        def value(n):
            return keep1[j, n] + recv1[j, n].astype(jnp.float32)

        out_z(j, value, part2, recv2, far2, mix2, s2_out, s2_in, c2_in, is_last(j))
        keep2[j] = value(z)

    def merge_y(j):
        merge(j, part2, recv2, far2, mix2, s2_out, s2_in, c2_in)

    def over_z(j):
        in_z(j, keep2, recv2, s2_in, jnp.logical_or(inner, is_last(j)))
        out[:, span(j)] = keep2[j].astype(jnp.bfloat16)

    def first_z(b):
        def value(n):
            return keep3[b, :, n]

        out_z(b, value, part3, recv3, far3, mix3, s3_out, s3_in, c3_in)
        own3[b] = value(z)

    def then_y(b):
        in_z(b, own3, recv3, s3_in, inner)
        part4[b] = own3[b, 1 - y].astype(jnp.bfloat16)
        remote(part4.at[b], recv4.at[b], s4_out, s4_in.at[b], y_side)

    def crossed_out(b, j):
        landed(recv4.at[b], s4_in.at[b])
        value = own3[b, y] + recv4[b].astype(jnp.float32)
        out[:, span(j)] = value.astype(jnp.bfloat16)

    fetch(0)
    finish(1 - y)
    ready(0)
    away(0, down_first(1 - y))
    fetch(1)
    finish(y)
    keep1[0] = down_first(y)

    def tell():
        count = tally[...]
        for i in range(3):
            landed(tally_in.at[i], t_in.at[i])
            count += tally_in[i]
        row = lax.dot_general(
            jnp.ones((8, rows), jnp.bfloat16), count.astype(jnp.bfloat16), nt,
            preferred_element_type=jnp.float32,
        )[0:1]
        spare = load - experts * row
        change = jnp.where(spare > 0.0, bias_rate, jnp.where(spare < 0.0, -bias_rate, 0.0))
        new_bias[...] = bias[...] + change
        counts[...] = row.astype(jnp.int32)

    lag_y, lag_m, lag_z = 2, 5, 13
    late = chunks - straight_chunks - 3

    def plain(j):
        ok = jnp.logical_and(j >= 0, j < chunks)
        for special in crossed:
            ok = jnp.logical_and(ok, j != special)
        return ok

    def step(j, carry):
        @pl.when(j < chunks)
        def _():
            ready(j)

            @pl.when(plain(j))
            def _():
                away(j, down(1 - y, j))

            for b, special in enumerate(crossed):

                @pl.when(j == special)
                def _(b=b):
                    keep3[b, 1 - y] = down(1 - y, j)

            @pl.when(j < chunks - 1)
            def _():
                fetch(j + 1)

            @pl.when(plain(j))
            def _():
                keep1[j] = down(y, j)

            for b, special in enumerate(crossed):

                @pl.when(j == special)
                def _(b=b):
                    keep3[b, y] = down(y, j)
                    first_z(b)

        pl.when(j == chunks)(tell)

        for lag, first, past in (
            (lag_m, 0, late), (lag_m - 1, late, chunks - straight_chunks)
        ):
            due = jnp.logical_and(j - lag >= first, j - lag < past)

            @pl.when(jnp.logical_and(plain(j - lag), due))
            def _(lag=lag):
                merge_y(j - lag)

        @pl.when(jnp.logical_and(plain(j - lag_y), j - lag_y < final))
        def _():
            over_y(j - lag_y)

        @pl.when(j - lag_y == final)
        def _():
            last_y(final)

        for b, special in enumerate(crossed):

            @pl.when(j == special + 5)
            def _(b=b):
                merge(b, part3, recv3, far3, mix3, s3_out, s3_in, c3_in)

            @pl.when(j == special + 8)
            def _(b=b):
                then_y(b)

            @pl.when(j == special + 11)
            def _(b=b, special=special):
                crossed_out(b, special)

        @pl.when(plain(j - lag_z))
        def _():
            over_z(j - lag_z)

        return carry

    lax.fori_loop(1, chunks + lag_z, step, 0)

    landed(gate_w.at[:, :, 1], m_out)
    landed(gate_w.at[:, :, 1], f_out)
    landed(tok.at[pl.ds(0, 2 * pieces - 1)], w_out.at[0])
    landed(tally_in, t_out)

    for sem in (d_out, md_out, fd_out):
        landed(down_w.at[:, 1, :, 0], sem)
    usual = pl.ds(0, chunks - len(crossed))
    landed(part1.at[usual], s1_out)
    landed(part2.at[usual], s2_out)
    landed(part3, s3_out)
    landed(part4, s4_out)

    passed(1, zs)

    @pl.when(end)
    def _():
        passed(0, 1)

    @pl.when(inner)
    def _():
        passed(0, zs + 1)


def group_scratch(zs, rows, top, width, ff, experts):
    slots = 2 * zs
    cd = width // chunks
    pieces = ff // lane_count
    twice = len(crossed)
    bf, f32 = jnp.bfloat16, jnp.float32
    return [
        ((top, rows), jnp.int32),
        ((top, rows), f32),
        ((1, experts), f32),
        ((slots, rows, width), bf),
        ((slots, 2 * experts, rows), f32),
        ((2, pieces, 2, lane_count, width), bf),
        ((2, pieces, 2, lane_count, width), bf),
        ((chunks, 2, pieces, 2, lane_count, cd), bf),
        ((pieces, slots, rows, 2 * lane_count), f32),
        ((slots, rows, 4 * ff), bf),
        ((2, zs * rows, 2 * lane_count), f32),
        ((chunks, zs, rows, cd), bf),
        ((chunks, zs, rows, cd), f32),
        ((chunks, zs, rows, cd), bf),
        ((chunks, zs - 1, rows, cd), bf),
        ((chunks, rows, cd), f32),
        ((chunks, zs - 1, rows, cd), bf),
        ((chunks, rows, cd), f32),
        ((chunks, rows, cd), bf),
        ((twice, 2, zs, rows, cd), f32),
        ((twice, zs - 1, 2, rows, cd), bf),
        ((twice, zs - 1, 2, rows, cd), bf),
        ((twice, 2, rows, cd), f32),
        ((twice, 2, rows, cd), f32),
        ((twice, 2, rows, cd), bf),
        ((twice, rows, cd), bf),
        ((twice, rows, cd), bf),
        ((2, zs * rows, cd), f32),
        ((experts, rows), f32),
        ((3, experts, rows), f32),
    ]


def finish_kernel(mixed, new_bias, counts, mixed_out, bias_out, counts_out, done):
    rows = mixed.shape[0] // copies
    moves = [
        (mixed.at[pl.ds(i * rows, rows)], mixed_out.at[pl.ds(i * rows, rows)])
        for i in range(copies)
    ]
    moves += [(new_bias, bias_out), (counts, counts_out)]
    moves = [pltpu.make_async_copy(a, b, done.at[i]) for i, (a, b) in enumerate(moves)]
    for move in moves:
        move.start()
    for move in moves:
        move.wait()


def group_body(zs, tokens, routes, route_weight, bias, w_gate, w_up, w_down):
    rows, width = tokens.shape
    experts = bias.shape[0]
    per_device, unit, _ = w_gate.shape
    ff = per_device * unit
    top = routes.shape[1]
    capacity = 5 * rows * top // (4 * experts)
    slots = 2 * zs
    pieces = ff // lane_count
    twice = len(crossed)
    dma = pltpu.SemaphoreType.DMA
    vmem = pl.BlockSpec(memory_space=pltpu.VMEM)
    anywhere = pl.BlockSpec(memory_space=pl.ANY)
    split = (pieces, lane_count, width)
    mean_load = rows * top * lax.axis_size("dp") * lax.axis_size("expert")
    results = pl.pallas_call(
        functools.partial(layer_kernel, zs, capacity, per_device, mean_load),
        out_shape=(
            pltpu.VMEM((rows, width), jnp.bfloat16),
            pltpu.VMEM((1, experts), jnp.float32),
            pltpu.VMEM((1, experts), jnp.int32),
        ),
        in_specs=[anywhere] * 7,
        out_specs=(vmem, vmem, vmem),
        scratch_shapes=[
            pltpu.VMEM(shape, kind)
            for shape, kind in group_scratch(zs, rows, top, width, ff, experts)
        ]
        + [
            dma((6,)), dma, dma((slots,)), dma((2,)), dma((slots,)), dma((2,)),
            dma((2, pieces)), dma((2,)), dma((chunks,)), dma, dma((2,)), dma, dma, dma,
            dma((2, pieces)), dma, dma((chunks,)), dma,
            dma((chunks,)), dma, dma((chunks,)), dma, dma((chunks,)),
            dma((twice,)), dma, dma((twice,)), dma((twice,)), dma,
            dma((zs,)), dma((3,)), dma, pltpu.SemaphoreType.REGULAR,
        ],
        compiler_params=pltpu.CompilerParams(
            collective_id=0, has_side_effects=True, vmem_limit_bytes=60000000
        ),
    )(
        tokens, routes.T, route_weight.T, bias.reshape(1, experts),
        w_gate.reshape(split), w_up.reshape(split), w_down.reshape(split),
    )
    results = [pltpu.with_memory_space_constraint(a, pltpu.VMEM) for a in results]
    mixed, new_bias, counts = pl.pallas_call(
        finish_kernel,
        out_shape=(
            jax.ShapeDtypeStruct((rows, width), jnp.bfloat16),
            jax.ShapeDtypeStruct((1, experts), jnp.float32),
            jax.ShapeDtypeStruct((1, experts), jnp.int32),
        ),
        in_specs=[vmem, vmem, vmem],
        out_specs=(anywhere, anywhere, anywhere),
        scratch_shapes=[dma((copies + 2,))],
    )(*results)
    return (mixed, new_bias.reshape(experts), counts.reshape(experts))


def body(tokens, routes, route_weight, bias, w_gate, w_up, w_down):
    rows, width = tokens.shape
    per_device, unit, _ = w_gate.shape
    ff = per_device * unit
    groups = lax.axis_size("expert")
    zs = groups // 2
    held = group_scratch(zs, rows, routes.shape[1], width, ff, bias.shape[0])
    total = 0
    for shape, kind in held:
        size = jnp.dtype(kind).itemsize
        for extent in shape:
            size *= extent
        total += size
    args = (tokens, routes, route_weight, bias, w_gate, w_up, w_down)
    fits = total < 0.85 * VMEM_BYTES and rows == lane_count
    even = ff % lane_count == 0 and width % (chunks * lane_count) == 0
    if lax.axis_size("dp") == 4 and groups % 2 == 0 and zs == 4 and fits and even:
        return group_body(zs, *args)
    return exchange_body(*args)


def solution(mesh):
    placed = (
        P(("dp", "expert"), None),
        P(("dp", "expert"), None),
        P(("dp", "expert"), None),
        P(),
        P("expert", "dp", None),
        P("expert", "dp", None),
        P("expert", "dp", None),
    )
    return jax.shard_map(
        body,
        mesh=mesh,
        in_specs=placed,
        out_specs=(P(("dp", "expert"), None), P(), P()),
        check_vma=False,
    )
```
